256 devices in a mesh: dom: 32 (over y, z), sub: 8 (over x, core).
Axes of the slice: x: 4, y: 4, z: 8, core: 2. Of those that a mesh axis runs over, the one named last changes fastest.
Arguments:
- positions: float32 [16384, 3, 256], P(('dom', 'sub')), may hold values from -6 to 6
- time_bins: int32 [16384, 256], P(('dom', 'sub')), may hold values from 0 to 5
- home_groups: int32 [16384], P(('dom', 'sub')), may hold values from 0 to 63
- targets: int32 [16384, 4], P(('dom', 'sub')), may hold values from -1 to 31, as said below
- target_groups: int32 [16384, 4], P(('dom', 'sub')), may hold values from 0 to 63
- node_pos: float32 [3, 1048576], P(None, ('dom', 'sub')), may hold values from -6 to 6
- node_mass: float32 [1048576], P(('dom', 'sub')), may hold values from 0.2 to 2
- node_lists: int32 [2048, 256], P('dom'), may hold values from 0 to 32767
- list_counts: int32 [2048], P('dom'), may hold values from 64 to 256, as said below
Outputs:
- forces: float32 [16384, 3, 256], P(('dom', 'sub'))
The draws below stay inside these ranges and needn't reach their ends.
Inputs may be any that keep to these rules, and one draw needn't show every extreme that they name: `targets`: row b names the remote domains that block b visits, each at most once and never its own domain b // 512; -1 marks an unused entry, in any column. The rows of one device name one domain at most 8 times, and some device names some domain exactly 8 times in every draw. The rows of one domain's 8 devices together name one domain at most 16 times, and this is reached in every draw. `list_counts`: each domain has at least one list with all 256 entries valid.
All inputs are finite; a program needn't handle non-finite values.
Results may differ from the reference program's by a relative error of at most 0.0003.
Values sent between devices are 32-bit elements; how exact they have to be, the bound alone decides.
No kernel may reach another device: no remote copies, remote signals or barrier semaphores. Data moves between devices by JAX's collectives and lax.ppermute only.
A program may use at most 128 MiB of HBM per device.

```python
import math
import jax
import jax.numpy as jnp
from jax import lax

BLOCK = 256
BLK_DEV = 64
TOP = 4
LIST = 256
GROUPS = 64
NODE_DEV = 4096
BINS = 6
CUR_BIN = 2
BLOCKS = 16384
NODES = 1048576
CAP = 8
CAP_ROW = 16
N_DOM = 32
N_SUB = 8


def draw_list_counts(key, part):
    count_key = jax.random.fold_in(key, 11)
    full_key = jax.random.fold_in(key, 12)
    counts = jax.random.randint(count_key, (N_DOM, GROUPS), LIST // 4, LIST + 1)
    full_list = jax.random.randint(full_key, (N_DOM,), 0, GROUPS)
    counts = jnp.where(jnp.arange(GROUPS)[None, :] == full_list[:, None], LIST, counts)
    return counts.reshape(N_DOM * GROUPS).astype(jnp.int32)


def draw_targets(key, part):
    hot_key = jax.random.fold_in(key, 21)
    order_key = jax.random.fold_in(key, 22)
    level_key = jax.random.fold_in(key, 23)
    wish_key = jax.random.fold_in(key, 24)
    block_key = jax.random.fold_in(key, 25)
    column_key = jax.random.fold_in(key, 26)
    hot_domain = jax.random.randint(hot_key, (), 0, N_DOM)
    domain_ids = jnp.arange(N_DOM, dtype=jnp.int32)
    orders = jax.vmap(lambda one_key: jax.random.permutation(one_key, N_SUB))(jax.random.split(order_key, N_DOM))
    levels = jax.random.randint(level_key, (N_DOM, N_SUB, 1), 0, 4)
    wishes = jnp.minimum(CAP, jax.random.randint(wish_key, (N_DOM, N_SUB, N_DOM), 0, CAP + 1) * levels // 2)
    wishes = jnp.where(domain_ids[None, None, :] == hot_domain, CAP, wishes)
    wishes = jnp.where(domain_ids[:, None, None] == domain_ids[None, None, :], 0, wishes).astype(jnp.int32)
    rotation = (hot_domain + domain_ids) % N_DOM
    unrotate = (domain_ids - hot_domain) % N_DOM
    budget = BLK_DEV * TOP

    def row_counts(row_wishes, row_order):

        def advance(already, position):
            wanted = jnp.minimum(row_wishes[row_order[position]], CAP_ROW - already)
            turned = wanted[rotation]
            before = jnp.cumsum(turned) - turned
            granted = jnp.maximum(jnp.minimum(turned, budget - before), 0)[unrotate]
            return (already + granted, granted)
        _, granted = lax.scan(advance, jnp.zeros((N_DOM,), jnp.int32), jnp.arange(N_SUB))
        return jnp.zeros((N_SUB, N_DOM), jnp.int32).at[row_order].set(granted)
    counts = jax.vmap(row_counts)(wishes, orders).reshape(N_DOM * N_SUB, N_DOM)
    tickets = jnp.arange(budget, dtype=jnp.int32)

    def device_table(device_counts, shuffle_key, order_keys):
        boundaries = jnp.cumsum(device_counts)
        ticket_domain = jnp.sum((boundaries[None, :] <= tickets[:, None]).astype(jnp.int32), axis=1)
        ticket_domain = jnp.where(tickets < boundaries[-1], ticket_domain, -1)
        assigned = ticket_domain.reshape(TOP, BLK_DEV).T
        assigned = assigned[jax.random.permutation(shuffle_key, BLK_DEV)]
        column_orders = jax.vmap(lambda one_key: jax.random.permutation(one_key, TOP))(jax.random.split(order_keys, BLK_DEV))
        return jnp.take_along_axis(assigned, column_orders, axis=1)
    device_total = N_DOM * N_SUB
    tables = jax.vmap(device_table)(counts, jax.random.split(block_key, device_total), jax.random.split(column_key, device_total))
    return tables.reshape(device_total * BLK_DEV, TOP).astype(jnp.int32)


def set_ends(array, own_key, smallest, largest):
    dims = array.shape
    index_at = [jax.random.randint(jax.random.fold_in(own_key, axis), (), 0, dims[axis]) for axis in range(len(dims))]
    array = array.at[tuple(index_at)].set(smallest)
    longest = dims.index(max(dims))
    index_at[longest] = (index_at[longest] + 1) % dims[longest]
    return array.at[tuple(index_at)].set(largest)


def shard_levels(stream_key, shape, cuts, smallest, largest):
    factor_of, own = 1.0, jax.random.fold_in(stream_key, 6)
    for axis_at, blocks in cuts:
        draws = jnp.exp(jax.random.uniform(jax.random.fold_in(own, axis_at), (blocks,), jnp.float32, smallest / len(cuts), largest / len(cuts)))
        factor_of = factor_of * jnp.repeat(draws, shape[axis_at] // blocks).reshape([-1 if axis == axis_at else 1 for axis in range(len(shape))])
    return factor_of


def bell_draw(key, extent, scale, most, pieces=(), kind=jnp.bfloat16):
    values = jax.random.normal(key, extent, jnp.float32) * scale
    if len(pieces) > 0:
        values = shard_levels(key, extent, pieces, -0.22, 0.18) * values
    return jnp.clip(values, min=-most, max=most).astype(kind)


def setup_inputs(seed: int = 0) -> dict:
    seeds = jax.random.split(jax.random.key(seed), 10)
    positions = bell_draw(seeds[0], (BLOCKS, 3, BLOCK), 1.0, 6.0, ((0, 256),), jnp.float32)
    time_bins = set_ends(jax.random.randint(seeds[1], (BLOCKS, BLOCK), 0, BINS), jax.random.fold_in(seeds[1], 1), 0, BINS - 1).astype(jnp.int32)
    home_groups = set_ends(jax.random.randint(seeds[2], (BLOCKS,), 0, GROUPS), jax.random.fold_in(seeds[2], 1), 0, GROUPS - 1).astype(jnp.int32)
    targets = draw_targets(jax.random.fold_in(seeds[9], 71), 0)
    target_groups = set_ends(jax.random.randint(seeds[4], (BLOCKS, TOP), 0, GROUPS), jax.random.fold_in(seeds[4], 1), 0, GROUPS - 1).astype(jnp.int32)
    node_pos = bell_draw(seeds[5], (3, NODES), 1.0, 6.0, ((1, 256),), jnp.float32)
    node_mass = jnp.clip(jnp.exp(math.log(2.0) - 2.3025851 * jax.random.uniform(seeds[6], (NODES,), jnp.float32) ** shard_levels(seeds[6], (NODES,), ((0, 256),), -0.2, 0.2)), 0.2, 2.0)
    node_lists = set_ends(jax.random.randint(seeds[7], (N_DOM * GROUPS, LIST), 0, NODE_DEV * N_SUB), jax.random.fold_in(seeds[7], 1), 0, (NODE_DEV * N_SUB) - 1).astype(jnp.int32)
    list_counts = draw_list_counts(jax.random.fold_in(seeds[9], 71), 0)
    return dict(positions=positions, time_bins=time_bins, home_groups=home_groups, targets=targets, target_groups=target_groups, node_pos=node_pos, node_mass=node_mass, node_lists=node_lists, list_counts=list_counts)


soften_sq = 0.04
gauss_slope = 1.1283791670955126

def short_pull(sink_pos, source_pos, source_mass):
    offset = sink_pos[:, None, :] - source_pos[:, :, None]
    range_sq = lax.optimization_barrier(jnp.sum(offset * offset, axis=0)) + soften_sq
    distance = jnp.sqrt(range_sq)
    scaled = distance * 0.5
    factor = lax.erfc(scaled) + gauss_slope * scaled * jnp.exp(-scaled * scaled)
    weight = source_mass[:, None] * factor / (range_sq * distance)
    return -lax.optimization_barrier(jnp.sum(offset * weight[None, :, :], axis=1))

def reference(positions, time_bins, home_groups, targets, target_groups, node_pos, node_mass, node_lists, list_counts):
    per_domain = BLK_DEV * N_SUB
    node_count = NODE_DEV * N_SUB
    block_ids = jnp.arange(BLOCKS, dtype=jnp.int32)
    home_domain = block_ids // per_domain
    visit_domain = jnp.concatenate([home_domain[:, None], jnp.maximum(targets, 0)], axis=1).astype(jnp.int32)
    visit_group = jnp.concatenate([home_groups[:, None], target_groups], axis=1).astype(jnp.int32)
    visit_alive = jnp.concatenate([jnp.ones((BLOCKS, 1), jnp.float32), (targets >= 0).astype(jnp.float32)], axis=1)
    list_rows = visit_domain * GROUPS + visit_group
    entry_ids = jnp.arange(LIST, dtype=jnp.int32)

    def one_visit(sink_pos, list_row, domain_id, is_alive):
        node_index = node_lists[list_row] + domain_id * node_count
        node_weight = node_mass[node_index] * (entry_ids < list_counts[list_row]).astype(jnp.float32) * is_alive
        return short_pull(sink_pos, node_pos[:, node_index], node_weight)

    def one_block(sink_pos, block_rows, block_domains, block_alive):
        pulls = jax.vmap(one_visit, in_axes=(None, 0, 0, 0))(sink_pos, block_rows, block_domains, block_alive)
        return lax.optimization_barrier(jnp.sum(pulls, axis=0))

    def one_group(operands):
        return jax.vmap(one_block)(*operands)
    grouped = lax.map(one_group, (positions.reshape(BLOCKS // 8, 8, 3, BLOCK), list_rows.reshape(BLOCKS // 8, 8, TOP + 1), visit_domain.reshape(BLOCKS // 8, 8, TOP + 1), visit_alive.reshape(BLOCKS // 8, 8, TOP + 1)))
    summed = grouped.reshape(BLOCKS, 3, BLOCK)
    active = (time_bins <= CUR_BIN).astype(jnp.float32)
    return summed * active[:, None, :]
```

```python
import functools
import math

import jax
import jax.numpy as jnp
from jax import lax
from jax.experimental import pallas as pl
from jax.experimental.pallas import tpu as pltpu
from jax.sharding import PartitionSpec as P

CUR_BIN = 2
SOFT = 0.04
F32 = jnp.float32
BF16 = jnp.bfloat16
I32 = jnp.int32

BETA = 0.3
POLY = (
    0.000177460321,
    0.334470999,
    0.374323182,
    0.116028516,
    0.555240376,
    -0.510157925,
    0.129925288,
)
LEAD = POLY[6]
MONIC = tuple(c / LEAD for c in POLY[:6])
TAIL = 1.0 / (BETA * math.sqrt(math.pi) * LEAD)
DECAY = -math.log2(math.e) / (4.0 * BETA * BETA)
OUT_SCALE = BETA * BETA * LEAD

WIDTHS = (128, 144, 160, 192, 256)
KI = 2
VMEM = pltpu.VMEM
SMEM = pltpu.SMEM
SLOTS = 8


def vspec():
    return pl.BlockSpec(memory_space=VMEM)


def sspec():
    return pl.BlockSpec(memory_space=SMEM)


def nt_dot(a, b):
    return lax.dot_general(a, b, (((1,), (1,)), ((), ())), preferred_element_type=F32)


def split3(v):
    first = v.astype(BF16).astype(F32)
    rest = v - first
    second = rest.astype(BF16).astype(F32)
    return first, second, rest - second


def request_kernel(targets_ref, groups_ref, counts_ref, pos_ref, mass_ref, req_ref, slot_ref, nodes_ref):
    pairs = targets_ref.shape[1]
    domains = req_ref.shape[0]
    dest = targets_ref[...].astype(F32)
    along = jnp.broadcast_to(dest, (pairs, pairs))
    down = jnp.transpose(along)
    earlier = lax.broadcasted_iota(I32, (pairs, pairs), 0) < lax.broadcasted_iota(I32, (pairs, pairs), 1)
    rank = jnp.sum(jnp.where((along == down) & earlier, 1.0, 0.0), axis=0, keepdims=True)
    slot = jnp.where(dest >= 0, dest * SLOTS + rank, -1.0)
    slot_ref[...] = slot.astype(I32)
    dom_id = lax.broadcasted_iota(I32, (domains, pairs), 0).astype(F32)
    asked = groups_ref[...].astype(F32) + 1.0
    by_dom = jnp.where(dom_id == dest, asked, 0.0).astype(BF16)
    lane_id = lax.broadcasted_iota(I32, (128, pairs), 0).astype(F32)
    by_rank = jnp.where(lane_id == rank, 1.0, 0.0).astype(BF16)
    wanted = nt_dot(by_dom, by_rank).astype(I32)
    half = counts_ref.shape[1]
    tail = jnp.concatenate([jnp.zeros((1, 128 - half), I32), counts_ref[...]], axis=1)
    lanes = lax.broadcasted_iota(I32, (domains, 128), 1)
    req_ref[...] = jnp.where(lanes < 128 - half, wanted, jnp.broadcast_to(tail, (domains, 128)))
    rows = nodes_ref.shape[2]
    for r in range(rows):
        for c in range(3):
            nodes_ref[0, c, r : r + 1, :] = pos_ref[c : c + 1, 128 * r : 128 * r + 128]
        nodes_ref[0, 3, r : r + 1, :] = mass_ref[0:1, 128 * r : 128 * r + 128]
    for c in range(4):
        tile = nodes_ref[0, c]
        for s in range(1, nodes_ref.shape[0]):
            nodes_ref[s, c] = tile


def list_kernel(req_ref, nodes_ref, lists_ref, counts_ref, tab_ref, reply_ref):
    sharers, _, rows, _ = nodes_ref.shape
    octets = lists_ref.shape[0] // 8

    def gather(i, carry):
        first = pl.multiple_of(i * 8, 8)
        for h in range(2):
            index = lists_ref[pl.ds(first, 8), 128 * h : 128 * h + 128]
            lane = index & 127
            row = index >> 7

            def one_share(s, accs):
                accs = list(accs)
                for r in range(rows):
                    here = row == s * rows + r
                    for c in range(4):
                        spread = jnp.broadcast_to(nodes_ref[s, c, r : r + 1, :], (8, 128))
                        picked = jnp.take_along_axis(spread, lane, axis=1, mode="promise_in_bounds")
                        accs[c] = jnp.where(here, picked, accs[c])
                return tuple(accs)

            zero = jnp.zeros((8, 128), F32)
            accs = lax.fori_loop(0, sharers, one_share, (zero,) * 4)
            entry = lax.broadcasted_iota(I32, (8, 128), 1) + 128 * h
            valid = entry < counts_ref[pl.ds(first, 8), :]
            for c in range(4):
                value = accs[c] * BETA if c < 3 else jnp.where(valid, accs[c], 0.0)
                for k in range(8):
                    tab_ref[first + k, 4 * h + c : 4 * h + c + 1, :] = value[k : k + 1, :]
        return carry

    lax.fori_loop(0, octets, gather, 0)

    def pack(d, carry):
        for j in range(SLOTS):
            group = jnp.maximum(req_ref[d, j] - 1, 0)
            reply_ref[d, j] = tab_ref[group]
        return carry

    lax.fori_loop(0, reply_ref.shape[0], pack, 0)


def row_masks():
    row = lax.broadcasted_iota(I32, (8, 128), 0)
    return row < 4, row % 4 == 3, row


def list_features(tile):
    low, last, row = row_masks()
    sq = tile * tile
    norm = pltpu.roll(sq, 1, 0) + pltpu.roll(sq, 2, 0) + pltpu.roll(sq, 3, 0)
    g = split3(jnp.where(last, norm, tile))
    ga = [pltpu.roll(v, 4, 0) for v in g]

    def pair(a, b, h):
        if h == 0:
            return jnp.where(low, g[a], ga[b])
        return jnp.where(low, ga[a], g[b])

    ones = jnp.where(row < 3, 1.0, 0.0)
    feats = jnp.concatenate(
        [
            jnp.concatenate([pair(0, 0, h), pair(0, 1, h), pair(1, 2, h), ones], axis=0)
            for h in range(2)
        ],
        axis=1,
    ).astype(BF16)
    m1, m2, m3 = pltpu.roll(tile, 7, 0), pltpu.roll(tile, 6, 0), pltpu.roll(tile, 5, 0)
    col = row % 4
    mass = jnp.where(col == 0, m3, jnp.where(col == 1, m2, m1))
    w = split3(jnp.where(last, tile, tile * mass))
    wa = [pltpu.roll(v, 4, 0) for v in w]
    zero = jnp.zeros((8, 128), F32)
    loaded = jnp.concatenate(
        [
            jnp.concatenate(
                [
                    jnp.where(low, w[0], wa[1]) if h == 0 else jnp.where(low, wa[0], w[1]),
                    jnp.where(low, w[2] if h == 0 else wa[2], zero),
                ],
                axis=0,
            )
            for h in range(2)
        ],
        axis=1,
    ).astype(BF16)
    return feats, loaded


def weights(s):
    q = lax.rsqrt(s)
    t = 1.0 / (s * q + 1.0)
    p = t + MONIC[5]
    for k in (4, 3, 2, 1, 0):
        p = p * t + MONIC[k]
    e = jnp.exp2(s * DECAY)
    return (q * q) * e * (q * p + TAIL)


def run_items(groups, blk_ref, row_ref, nact_ref, fc_ref, tab_ref, acc_ref, bufs):
    last_block = fc_ref.shape[0] - 1

    def items(g):
        return [g * KI + k for k in range(KI)]

    def widest(g):
        n = I32(0)
        for i in items(g):
            n = jnp.maximum(n, nact_ref[jnp.minimum(blk_ref[i], last_block)])
        return n

    def prepare(g, par, width):
        s_bufs, y_bufs = bufs
        for k, i in enumerate(items(g)):
            b = jnp.minimum(blk_ref[i], last_block)
            feats, loaded = list_features(tab_ref[row_ref[i]])
            y_bufs[par][k][...] = loaded
            s_bufs[par][k][:width, :] = jnp.dot(
                fc_ref[b, :width, :], feats, preferred_element_type=F32
            )

    def reduce(g, par, width):
        s_bufs, y_bufs = bufs
        for k, i in enumerate(items(g)):
            w = weights(s_bufs[par][k][:width, :])
            hi = w.astype(BF16)
            lo = (w - hi.astype(F32)).astype(BF16)
            loaded = y_bufs[par][k][...]
            b = blk_ref[i]
            acc_ref[b, :, :width] = acc_ref[b, :, :width] + (nt_dot(loaded, hi) + nt_dot(loaded, lo))

    def by_width(n, body):
        low = -1
        for width in WIDTHS:
            @pl.when((n > low) & (n <= width))
            def _(width=width):
                body(width)
            low = width

    def step(g, par):
        n = jnp.maximum(widest(g), widest(g + 1))

        def body(width):
            prepare(g + 1, 1 - par, width)
            reduce(g, par, width)

        by_width(n, body)

    prepare(0, 0, 256)

    def pair(gg, carry):
        step(2 * gg, 0)
        step(2 * gg + 1, 1)
        return carry

    lax.fori_loop(0, (groups + 1) // 2, pair, 0)


def buffers():
    return (
        [VMEM((256, 256), F32) for _ in range(2 * KI)],
        [VMEM((16, 256), BF16) for _ in range(2 * KI)],
    )


def take_buffers(flat):
    s = flat[: 2 * KI]
    y = flat[2 * KI :]
    return [s[:KI], s[KI:]], [y[:KI], y[KI:]]


PAD = 4 * KI


def home_kernel(
    home_ref, slot_ref, nact_ref, pos_ref, bins_ref, tab_ref, fc_ref, key_ref, acc_ref, blk_out, row_out, n_out, blk_ref, row_ref, *flat
):
    blocks = pos_ref.shape[0]
    width = pos_ref.shape[2]
    active = bins_ref[...] <= CUR_BIN
    tri = lax.broadcasted_iota(I32, (width, width), 0) <= lax.broadcasted_iota(I32, (width, width), 1)
    upto = jnp.dot(
        jnp.where(active, 1.0, 0.0).astype(BF16),
        jnp.where(tri, 1.0, 0.0).astype(BF16),
        preferred_element_type=F32,
    )
    key_ref[...] = jnp.where(active, upto - 1.0, -1.0).astype(I32)

    low8 = lax.broadcasted_iota(I32, (8, width), 0) < 4
    row8 = lax.broadcasted_iota(I32, (8, width), 0)

    def compact(bb, carry):
        for u in range(4):
            b = bb * 4 + u
            key = jnp.broadcast_to(key_ref[pl.ds(b, 1), :], (width, width))
            chosen = jnp.where(lax.broadcasted_iota(I32, (width, width), 0) == key, 1.0, 0.0).astype(BF16)
            pos = jnp.concatenate([pos_ref[b] * BETA, jnp.zeros((5, width), F32)], axis=0)
            parts = jnp.concatenate(split3(pos), axis=0).astype(BF16)
            moved = nt_dot(parts, chosen)
            x = (moved[0:8] + moved[8:16]) + moved[16:24]
            sq = x * x
            norm = sq[0:1] + sq[1:2] + sq[2:3] + SOFT * BETA * BETA
            n1, n2, n3 = split3(norm)
            a1, a2, a3 = split3(x * -2.0)
            unit = jnp.where(row8 == 3, 1.0, 0.0)
            a1 = a1 + unit
            r1, r2 = pltpu.roll(a1, 4, 0), pltpu.roll(a2, 4, 0)
            feats = jnp.concatenate(
                [
                    jnp.where(low8, a1, r2),
                    jnp.where(low8, a3, r1),
                    jnp.where(low8, a2, r1),
                    jnp.concatenate([n1, n2, n3, jnp.zeros((5, width), F32)], axis=0),
                ],
                axis=0,
            )
            fc_ref[b] = jnp.transpose(feats).astype(BF16)
            acc_ref[b] = jnp.zeros((16, width), F32)
        return carry

    lax.fori_loop(0, blocks // 4, compact, 0)
    acc_ref[blocks] = jnp.zeros((16, width), F32)

    def home_item(i, carry):
        inside = i < blocks
        blk_ref[i] = jnp.where(inside, i, blocks)
        row_ref[i] = jnp.where(inside, home_ref[jnp.minimum(i, blocks - 1)], 0)
        return carry

    lax.fori_loop(0, blocks + PAD, home_item, 0)
    run_items(blocks // KI, blk_ref, row_ref, nact_ref, fc_ref, tab_ref, acc_ref, take_buffers(flat))

    pairs = slot_ref.shape[1]
    per_block = pairs // blocks

    def visit(i, n):
        slot = slot_ref[0, i]

        @pl.when(slot >= 0)
        def _():
            blk_out[n] = i // per_block
            row_out[n] = slot

        return n + jnp.where(slot >= 0, 1, 0)

    count = lax.fori_loop(0, pairs, visit, I32(0))

    def pad_item(k, carry):
        blk_out[count + k] = blocks
        row_out[count + k] = 0
        return carry

    lax.fori_loop(0, PAD, pad_item, 0)
    n_out[0] = count


def remote_kernel(n_ref, blk_ref, row_ref, nact_ref, fc_ref, tab_ref, acc_in_ref, key_ref, pos_ref, out_ref, acc_ref, *flat):
    blocks = pos_ref.shape[0]
    acc_ref[...] = acc_in_ref[...]
    run_items((n_ref[0] + KI - 1) // KI, blk_ref, row_ref, nact_ref, fc_ref, tab_ref, acc_ref, take_buffers(flat))

    def finish(bb, carry):
        for u in range(4):
            b = bb * 4 + u
            acc = acc_ref[b]
            top = acc[0:8]
            total = top + pltpu.roll(top, 4, 0) + acc[8:16]
            key = key_ref[pl.ds(b, 1), :]
            parts = []
            for h in range(2):
                at = jnp.broadcast_to(key[:, 128 * h : 128 * h + 128], (8, 128))
                lane = at & 127
                left = jnp.take_along_axis(total[:, :128], lane, axis=1, mode="promise_in_bounds")
                right = jnp.take_along_axis(total[:, 128:], lane, axis=1, mode="promise_in_bounds")
                parts.append(jnp.where(at < 128, left, right))
            back = jnp.concatenate(parts, axis=1)
            pull = (back[0:3] - pos_ref[b] * (BETA * back[3:4])) * OUT_SCALE
            out_ref[b] = jnp.where(key >= 0, pull, 0.0)
        return carry

    lax.fori_loop(0, blocks // 4, finish, 0)


def local(positions, time_bins, home_groups, targets, target_groups, node_pos, node_mass, node_lists, list_counts):
    domains = lax.axis_size("dom")
    sharers = lax.axis_size("sub")
    blocks, most = targets.shape
    pairs = blocks * most
    width = positions.shape[2]
    lists = node_lists.shape[0]
    rows = node_mass.shape[0] // 128

    req, slot, nodes = pl.pallas_call(
        request_kernel,
        out_shape=(
            jax.ShapeDtypeStruct((domains, 128), I32),
            jax.ShapeDtypeStruct((1, pairs), I32),
            jax.ShapeDtypeStruct((sharers, 4, rows, 128), F32),
        ),
        in_specs=[vspec()] * 5,
        out_specs=(vspec(),) * 3,
        name="requests",
    )(
        targets.reshape(1, pairs),
        target_groups.reshape(1, pairs),
        list_counts.reshape(1, lists),
        node_pos,
        node_mass.reshape(1, -1),
    )
    nodes = lax.all_to_all(nodes, "sub", 0, 0, tiled=True)
    req = lax.all_to_all(req.reshape(domains, 1, 128), "dom", 0, 0, tiled=True).reshape(domains, 128)
    nact = jnp.sum((time_bins <= CUR_BIN).astype(I32), axis=1)

    tab, reply = pl.pallas_call(
        list_kernel,
        out_shape=(
            jax.ShapeDtypeStruct((lists, 8, 128), F32),
            jax.ShapeDtypeStruct((domains, SLOTS, 8, 128), F32),
        ),
        in_specs=[sspec(), vspec(), vspec(), vspec()],
        out_specs=(vspec(),) * 2,
        name="lists",
    )(req, nodes, node_lists, list_counts.reshape(lists, 1))

    reply = lax.all_to_all(reply.reshape(domains, SLOTS * 8, 128), "dom", 0, 0, tiled=True)

    s_bufs, y_bufs = buffers()
    room = pairs + PAD
    fc, key, acc, blk, row, n = pl.pallas_call(
        home_kernel,
        out_shape=(
            jax.ShapeDtypeStruct((blocks, width, 32), BF16),
            jax.ShapeDtypeStruct((blocks, width), I32),
            jax.ShapeDtypeStruct((blocks + 1, 16, width), F32),
            jax.ShapeDtypeStruct((room,), I32),
            jax.ShapeDtypeStruct((room,), I32),
            jax.ShapeDtypeStruct((8,), I32),
        ),
        in_specs=[sspec(), sspec(), sspec(), vspec(), vspec(), vspec()],
        out_specs=(vspec(),) * 3 + (sspec(),) * 3,
        scratch_shapes=[SMEM((blocks + PAD,), I32), SMEM((blocks + PAD,), I32), *s_bufs, *y_bufs],
        cost_estimate=pl.CostEstimate(flops=40_000_000, bytes_accessed=4_000_000, transcendentals=12_000_000),
        name="home_pulls",
    )(home_groups, slot, nact, positions, time_bins, tab)

    return pl.pallas_call(
        remote_kernel,
        out_shape=jax.ShapeDtypeStruct((blocks, 3, width), F32),
        in_specs=[sspec()] * 4 + [vspec()] * 5,
        out_specs=vspec(),
        scratch_shapes=[VMEM((blocks + 1, 16, width), F32), *s_bufs, *y_bufs],
        name="remote_pulls",
    )(n, blk, row, nact, fc, reply.reshape(domains * SLOTS, 8, 128), acc, key, positions)


def solution(mesh):
    return jax.shard_map(
        local,
        mesh=mesh,
        in_specs=(
            P(("dom", "sub"), None, None),
            P(("dom", "sub"), None),
            P(("dom", "sub")),
            P(("dom", "sub"), None),
            P(("dom", "sub"), None),
            P(None, ("dom", "sub")),
            P(("dom", "sub")),
            P("dom", None),
            P("dom"),
        ),
        out_specs=P(("dom", "sub"), None, None),
        check_vma=False,
    )
```

```python
import functools
import math

import jax
import jax.numpy as jnp
from jax import lax
from jax.experimental import pallas as pl
from jax.experimental.pallas import tpu as pltpu
from jax.sharding import PartitionSpec as P

CUR_BIN = 2
SOFT = 0.04
F32 = jnp.float32
BF16 = jnp.bfloat16
I32 = jnp.int32

BETA = 0.3
POLY = (
    0.000177460321,
    0.334470999,
    0.374323182,
    0.116028516,
    0.555240376,
    -0.510157925,
    0.129925288,
)
LEAD = POLY[6]
MONIC = tuple(c / LEAD for c in POLY[:6])
TAIL = 1.0 / (BETA * math.sqrt(math.pi) * LEAD)
DECAY = -math.log2(math.e) / (4.0 * BETA * BETA)
OUT_SCALE = BETA * BETA * LEAD

WIDTHS = (128, 144, 160, 192, 256)
KI = 2
VMEM = pltpu.VMEM
SMEM = pltpu.SMEM
SLOTS = 8


def vspec():
    return pl.BlockSpec(memory_space=VMEM)


def sspec():
    return pl.BlockSpec(memory_space=SMEM)


def nt_dot(a, b):
    return lax.dot_general(a, b, (((1,), (1,)), ((), ())), preferred_element_type=F32)


def split3(v):
    first = v.astype(BF16).astype(F32)
    rest = v - first
    second = rest.astype(BF16).astype(F32)
    return first, second, rest - second


def request_kernel(targets_ref, groups_ref, counts_ref, pos_ref, mass_ref, req_ref, slot_ref, nodes_ref):
    most = targets_ref.shape[0]
    pairs = most * targets_ref.shape[1]
    domains = req_ref.shape[0]

    def in_line(ref):
        return jnp.concatenate([ref[v : v + 1, :] for v in range(most)], axis=1).astype(F32)

    dest = in_line(targets_ref)
    along = jnp.broadcast_to(dest, (pairs, pairs))
    down = jnp.transpose(along)
    earlier = lax.broadcasted_iota(I32, (pairs, pairs), 0) < lax.broadcasted_iota(I32, (pairs, pairs), 1)
    rank = jnp.sum(jnp.where((along == down) & earlier, 1.0, 0.0), axis=0, keepdims=True)
    slot = jnp.where(dest >= 0, dest * SLOTS + rank, -1.0)
    slot_ref[...] = slot.astype(I32)
    dom_id = lax.broadcasted_iota(I32, (domains, pairs), 0).astype(F32)
    asked = in_line(groups_ref) + 1.0
    by_dom = jnp.where(dom_id == dest, asked, 0.0).astype(BF16)
    lane_id = lax.broadcasted_iota(I32, (128, pairs), 0).astype(F32)
    by_rank = jnp.where(lane_id == rank, 1.0, 0.0).astype(BF16)
    wanted = nt_dot(by_dom, by_rank).astype(I32)
    half = counts_ref.shape[1]
    tail = jnp.concatenate([jnp.zeros((1, 128 - half), I32), counts_ref[...]], axis=1)
    lanes = lax.broadcasted_iota(I32, (domains, 128), 1)
    req_ref[...] = jnp.where(lanes < 128 - half, wanted, jnp.broadcast_to(tail, (domains, 128)))
    rows = nodes_ref.shape[2]
    for r in range(rows):
        for c in range(3):
            nodes_ref[0, c, r : r + 1, :] = pos_ref[c : c + 1, 128 * r : 128 * r + 128]
        nodes_ref[0, 3, r : r + 1, :] = mass_ref[0:1, 128 * r : 128 * r + 128]
    for c in range(4):
        tile = nodes_ref[0, c]
        for s in range(1, nodes_ref.shape[0]):
            nodes_ref[s, c] = tile


def list_kernel(nodes_ref, lists_ref, counts_ref, tab_ref, table_ref, lane_ref):
    sharers, _, rows, _ = nodes_ref.shape
    total = sharers * rows
    octets = lists_ref.shape[0] // 8
    for c in range(3):
        tall = jnp.concatenate([nodes_ref[s, c] for s in range(sharers)], axis=0)
        parts = split3(jnp.transpose(tall) * BETA)
        for k in range(3):
            table_ref[128 * c : 128 * c + 128, total * k : total * k + total] = parts[k].astype(BF16)
    lane_ref[...] = lists_ref[...] & 127
    row_iota = lax.broadcasted_iota(I32, (total, 256), 0)
    lane_iota = lax.broadcasted_iota(I32, (128, 256), 0)
    entry_id = lax.broadcasted_iota(I32, (1, 256), 1)

    def gather(i, carry):
        first = pl.multiple_of(i * 8, 8)
        lane = [lane_ref[pl.ds(first, 8), 128 * h : 128 * h + 128] for h in range(2)]
        row = [lists_ref[pl.ds(first, 8), 128 * h : 128 * h + 128] >> 7 for h in range(2)]

        def one_share(s, accs):
            accs = list(accs)
            for r in range(rows):
                spread = jnp.broadcast_to(nodes_ref[s, 3, r : r + 1, :], (8, 128))
                for h in range(2):
                    picked = jnp.take_along_axis(spread, lane[h], axis=1, mode="promise_in_bounds")
                    accs[h] = jnp.where(row[h] == s * rows + r, picked, accs[h])
            one = first + s
            index = lists_ref[pl.ds(one, 1), :]
            chosen = jnp.where(row_iota == (index >> 7), 1.0, 0.0).astype(BF16)
            found = jnp.dot(
                table_ref[...], jnp.concatenate([chosen] * 3, axis=0), preferred_element_type=F32
            )
            here = lane_iota == (index & 127)
            valid = entry_id < counts_ref[one]
            for c in range(3):
                value = jnp.sum(
                    jnp.where(here, found[128 * c : 128 * c + 128, :], 0.0), axis=0, keepdims=True
                )
                value = jnp.where(valid, value, 0.0)
                for h in range(2):
                    tab_ref[one, 4 * h + c : 4 * h + c + 1, :] = value[:, 128 * h : 128 * h + 128]
            return tuple(accs)

        zero = jnp.zeros((8, 128), F32)
        accs = lax.fori_loop(0, sharers, one_share, (zero,) * 2)
        for k in range(8):
            for h in range(2):
                value = accs[h][k : k + 1, :]
                keep = entry_id[:, 128 * h : 128 * h + 128] < counts_ref[first + k]
                tab_ref[first + k, 4 * h + 3 : 4 * h + 4, :] = jnp.where(keep, value, 0.0)
        return carry

    lax.fori_loop(0, octets, gather, 0)


def pack_kernel(req_ref, tab_ref, reply_ref):
    def pack(d, carry):
        for j in range(SLOTS):
            group = jnp.maximum(req_ref[d, j] - 1, 0)
            reply_ref[d, j] = tab_ref[group]
        return carry

    lax.fori_loop(0, reply_ref.shape[0], pack, 0)


def row_masks():
    row = lax.broadcasted_iota(I32, (8, 128), 0)
    return row < 4, row % 4 == 3, row


def list_features(tile):
    low, last, row = row_masks()
    sq = tile * tile
    norm = pltpu.roll(sq, 1, 0) + pltpu.roll(sq, 2, 0) + pltpu.roll(sq, 3, 0)
    g = split3(jnp.where(last, norm, tile))
    ga = [pltpu.roll(v, 4, 0) for v in g]

    def pair(a, b, h):
        if h == 0:
            return jnp.where(low, g[a], ga[b])
        return jnp.where(low, ga[a], g[b])

    ones = jnp.where(row < 3, 1.0, 0.0)
    feats = jnp.concatenate(
        [
            jnp.concatenate([pair(0, 0, h), pair(0, 1, h), pair(1, 2, h), ones], axis=0)
            for h in range(2)
        ],
        axis=1,
    ).astype(BF16)
    m1, m2, m3 = pltpu.roll(tile, 7, 0), pltpu.roll(tile, 6, 0), pltpu.roll(tile, 5, 0)
    col = row % 4
    mass = jnp.where(col == 0, m3, jnp.where(col == 1, m2, m1))
    w = split3(jnp.where(last, tile, tile * mass))
    wa = [pltpu.roll(v, 4, 0) for v in w]
    zero = jnp.zeros((8, 128), F32)
    loaded = jnp.concatenate(
        [
            jnp.concatenate(
                [
                    jnp.where(low, w[0], wa[1]) if h == 0 else jnp.where(low, wa[0], w[1]),
                    jnp.where(low, w[2] if h == 0 else wa[2], zero),
                ],
                axis=0,
            )
            for h in range(2)
        ],
        axis=1,
    ).astype(BF16)
    return feats, loaded


def weights(s):
    q = lax.rsqrt(s)
    t = 1.0 / (s * q + 1.0)
    p = t + MONIC[5]
    for k in (4, 3, 2, 1, 0):
        p = p * t + MONIC[k]
    e = jnp.exp2(s * DECAY)
    return (q * q) * e * (q * p + TAIL)


def run_items(groups, blk_ref, row_ref, nact_ref, fc_ref, tab_ref, acc_ref, bufs):
    last_block = fc_ref.shape[0] - 1
    s_bufs, w_bufs, y_bufs = bufs

    def items(g):
        return [(g + 1) * KI + k for k in range(KI)]

    def widest(g):
        n = I32(0)
        for i in items(g):
            n = jnp.maximum(n, nact_ref[jnp.minimum(blk_ref[i], last_block)])
        return n

    def prepare(g, par, width):
        for k, i in enumerate(items(g)):
            b = jnp.minimum(blk_ref[i], last_block)
            feats, loaded = list_features(tab_ref[row_ref[i]])
            y_bufs[par][k][...] = loaded
            s_bufs[par][k][:width, :] = jnp.dot(
                fc_ref[b, :width, :], feats, preferred_element_type=F32
            )

    def weigh(par, width):
        for k in range(KI):
            w = weights(s_bufs[par][k][:width, :])
            hi = w.astype(BF16)
            w_bufs[par][k][0, :width, :] = hi
            w_bufs[par][k][1, :width, :] = (w - hi.astype(F32)).astype(BF16)

    def reduce(g, par, width):
        made = []
        for k in range(KI):
            loaded = y_bufs[par][k][...]
            made.append(
                nt_dot(loaded, w_bufs[par][k][0, :width, :]) + nt_dot(loaded, w_bufs[par][k][1, :width, :])
            )
        return made

    def add(g, made, width):
        for k, i in enumerate(items(g)):
            b = blk_ref[i]
            acc_ref[b, :, :width] = acc_ref[b, :, :width] + made[k]

    def by_width(n, body):
        low = -1
        for width in WIDTHS:
            @pl.when((n > low) & (n <= width))
            def _(width=width):
                body(width)
            low = width

    def step(g, par):
        n = jnp.maximum(jnp.maximum(widest(g), widest(g + 1)), widest(g - 1))

        def body(width):
            made = reduce(g - 1, 1 - par, width)
            prepare(g + 1, 1 - par, width)
            weigh(par, width)
            add(g - 1, made, width)

        by_width(n, body)

    for k in range(KI):
        w_bufs[1][k][...] = jnp.zeros(w_bufs[1][k].shape, BF16)
        y_bufs[1][k][...] = jnp.zeros(y_bufs[1][k].shape, BF16)
    prepare(0, 0, 256)

    def pair(gg, carry):
        step(2 * gg, 0)
        step(2 * gg + 1, 1)
        return carry

    lax.fori_loop(0, (groups + 2) // 2, pair, 0)


def buffers():
    return (
        *[VMEM((256, 256), F32) for _ in range(2 * KI)],
        *[VMEM((2, 256, 256), BF16) for _ in range(2 * KI)],
        *[VMEM((16, 256), BF16) for _ in range(2 * KI)],
    )


def take_buffers(flat):
    n = 2 * KI
    return [[flat[j * n : j * n + KI], flat[j * n + KI : j * n + n]] for j in range(3)]


PAD = 6 * KI


def home_kernel(
    home_ref, slot_ref, nact_ref, pos_ref, bins_ref, tab_ref, fc_ref, key_ref, acc_ref, blk_out, row_out, n_out, blk_ref, row_ref, *flat
):
    _, blocks, width = pos_ref.shape
    active = bins_ref[...] <= CUR_BIN
    tri = lax.broadcasted_iota(I32, (width, width), 0) <= lax.broadcasted_iota(I32, (width, width), 1)
    upto = jnp.dot(
        jnp.where(active, 1.0, 0.0).astype(BF16),
        jnp.where(tri, 1.0, 0.0).astype(BF16),
        preferred_element_type=F32,
    )
    key_ref[...] = jnp.where(active, upto - 1.0, -1.0).astype(I32)

    low8 = lax.broadcasted_iota(I32, (8, width), 0) < 4
    row8 = lax.broadcasted_iota(I32, (8, width), 0)

    def compact(bb, carry):
        for u in range(4):
            b = bb * 4 + u
            key = jnp.broadcast_to(key_ref[pl.ds(b, 1), :], (width, width))
            chosen = jnp.where(lax.broadcasted_iota(I32, (width, width), 0) == key, 1.0, 0.0).astype(BF16)
            pos = jnp.concatenate(
                [pos_ref[c, pl.ds(b, 1), :] * BETA for c in range(3)] + [jnp.zeros((5, width), F32)], axis=0
            )
            parts = jnp.concatenate(split3(pos), axis=0).astype(BF16)
            moved = nt_dot(parts, chosen)
            x = (moved[0:8] + moved[8:16]) + moved[16:24]
            sq = x * x
            norm = sq[0:1] + sq[1:2] + sq[2:3] + SOFT * BETA * BETA
            n1, n2, n3 = split3(norm)
            a1, a2, a3 = split3(x * -2.0)
            unit = jnp.where(row8 == 3, 1.0, 0.0)
            a1 = a1 + unit
            r1, r2 = pltpu.roll(a1, 4, 0), pltpu.roll(a2, 4, 0)
            feats = jnp.concatenate(
                [
                    jnp.where(low8, a1, r2),
                    jnp.where(low8, a3, r1),
                    jnp.where(low8, a2, r1),
                    jnp.concatenate([n1, n2, n3, jnp.zeros((5, width), F32)], axis=0),
                ],
                axis=0,
            )
            fc_ref[b] = jnp.transpose(feats).astype(BF16)
            acc_ref[b] = jnp.zeros((16, width), F32)
        return carry

    lax.fori_loop(0, blocks // 4, compact, 0)
    acc_ref[blocks] = jnp.zeros((16, width), F32)

    def home_item(i, carry):
        inside = (i >= KI) & (i < blocks + KI)
        b = jnp.clip(i - KI, 0, blocks - 1)
        blk_ref[i] = jnp.where(inside, b, blocks)
        row_ref[i] = jnp.where(inside, home_ref[b], 0)
        return carry

    lax.fori_loop(0, blocks + PAD, home_item, 0)
    run_items(blocks // KI, blk_ref, row_ref, nact_ref, fc_ref, tab_ref, acc_ref, take_buffers(flat))

    most = slot_ref.shape[1] // blocks

    def no_item(k, carry):
        blk_out[k] = blocks
        row_out[k] = 0
        return carry

    lax.fori_loop(0, KI, no_item, 0)

    def visits(b, n):
        for v in range(most):
            slot = slot_ref[0, v * blocks + b]
            blk_out[n] = b
            row_out[n] = jnp.maximum(slot, 0)
            n = n + jnp.where(slot >= 0, 1, 0)
        return n

    end = lax.fori_loop(0, blocks, visits, I32(KI))
    lax.fori_loop(end, end + PAD - KI, no_item, 0)
    n_out[0] = end - KI


def remote_kernel(n_ref, blk_ref, row_ref, nact_ref, fc_ref, tab_ref, acc_in_ref, key_ref, pos_ref, out_ref, acc_ref, *flat):
    blocks = pos_ref.shape[1]
    acc_ref[...] = acc_in_ref[...]
    run_items((n_ref[0] + KI - 1) // KI, blk_ref, row_ref, nact_ref, fc_ref, tab_ref, acc_ref, take_buffers(flat))

    def finish(bb, carry):
        for u in range(4):
            b = bb * 4 + u
            acc = acc_ref[b]
            top = acc[0:8]
            total = top + pltpu.roll(top, 4, 0) + acc[8:16]
            key = key_ref[pl.ds(b, 1), :]
            parts = []
            for h in range(2):
                at = jnp.broadcast_to(key[:, 128 * h : 128 * h + 128], (8, 128))
                lane = at & 127
                left = jnp.take_along_axis(total[:, :128], lane, axis=1, mode="promise_in_bounds")
                right = jnp.take_along_axis(total[:, 128:], lane, axis=1, mode="promise_in_bounds")
                parts.append(jnp.where(at < 128, left, right))
            back = jnp.concatenate(parts, axis=1)
            for c in range(3):
                pull = (back[c : c + 1] - pos_ref[c, pl.ds(b, 1), :] * (BETA * back[3:4])) * OUT_SCALE
                out_ref[c, pl.ds(b, 1), :] = jnp.where(key >= 0, pull, 0.0)
        return carry

    lax.fori_loop(0, blocks // 4, finish, 0)


def local(positions, time_bins, home_groups, targets, target_groups, node_pos, node_mass, node_lists, list_counts):
    domains = lax.axis_size("dom")
    sharers = lax.axis_size("sub")
    blocks, most = targets.shape
    pairs = blocks * most
    width = positions.shape[2]
    lists = node_lists.shape[0]
    rows = node_mass.shape[0] // 128

    req, slot, nodes = pl.pallas_call(
        request_kernel,
        out_shape=(
            jax.ShapeDtypeStruct((domains, 128), I32),
            jax.ShapeDtypeStruct((1, pairs), I32),
            jax.ShapeDtypeStruct((sharers, 4, rows, 128), F32),
        ),
        in_specs=[vspec()] * 5,
        out_specs=(vspec(),) * 3,
        compiler_params=pltpu.CompilerParams(vmem_limit_bytes=8 << 20),
        name="requests",
    )(targets.T, target_groups.T, list_counts.reshape(1, lists), node_pos, node_mass.reshape(1, -1))
    nodes = lax.all_to_all(nodes, "sub", 0, 0, tiled=True)
    req = lax.all_to_all(req.reshape(domains, 1, 128), "dom", 0, 0, tiled=True).reshape(domains, 128)
    nact = jnp.sum((time_bins <= CUR_BIN).astype(I32), axis=1)

    tab = pl.pallas_call(
        list_kernel,
        out_shape=jax.ShapeDtypeStruct((lists, 8, 128), F32),
        in_specs=[vspec(), vspec(), sspec()],
        out_specs=vspec(),
        scratch_shapes=[VMEM((384, 3 * sharers * rows), BF16), VMEM(node_lists.shape, I32)],
        compiler_params=pltpu.CompilerParams(vmem_limit_bytes=12 << 20),
        cost_estimate=pl.CostEstimate(flops=20_000_000, bytes_accessed=1_000_000, transcendentals=0),
        name="lists",
    )(nodes, node_lists, list_counts)

    reply = pl.pallas_call(
        pack_kernel,
        out_shape=jax.ShapeDtypeStruct((domains, SLOTS, 8, 128), F32),
        in_specs=[sspec(), vspec()],
        out_specs=vspec(),
        compiler_params=pltpu.CompilerParams(vmem_limit_bytes=8 << 20),
        name="pack",
    )(req, tab)
    reply = lax.all_to_all(reply.reshape(domains, SLOTS * 8, 128), "dom", 0, 0, tiled=True)

    positions = jnp.transpose(positions, (1, 0, 2))
    room = pairs + PAD
    fc, key, acc, blk, row, n = pl.pallas_call(
        home_kernel,
        out_shape=(
            jax.ShapeDtypeStruct((blocks, width, 32), BF16),
            jax.ShapeDtypeStruct((blocks, width), I32),
            jax.ShapeDtypeStruct((blocks + 1, 16, width), F32),
            jax.ShapeDtypeStruct((room,), I32),
            jax.ShapeDtypeStruct((room,), I32),
            jax.ShapeDtypeStruct((8,), I32),
        ),
        in_specs=[sspec(), sspec(), sspec(), vspec(), vspec(), vspec()],
        out_specs=(vspec(),) * 3 + (sspec(),) * 3,
        scratch_shapes=[SMEM((blocks + PAD,), I32), SMEM((blocks + PAD,), I32), *buffers()],
        compiler_params=pltpu.CompilerParams(vmem_limit_bytes=24 << 20),
        cost_estimate=pl.CostEstimate(flops=40_000_000, bytes_accessed=4_000_000, transcendentals=12_000_000),
        name="home_pulls",
    )(home_groups, slot, nact, positions, time_bins, tab)

    out = pl.pallas_call(
        remote_kernel,
        out_shape=jax.ShapeDtypeStruct((3, blocks, width), F32),
        in_specs=[sspec()] * 4 + [vspec()] * 5,
        out_specs=vspec(),
        scratch_shapes=[VMEM((blocks + 1, 16, width), F32), *buffers()],
        compiler_params=pltpu.CompilerParams(vmem_limit_bytes=24 << 20),
        name="remote_pulls",
    )(n, blk, row, nact, fc, reply.reshape(domains * SLOTS, 8, 128), acc, key, positions)
    return jnp.transpose(out, (1, 0, 2))


def solution(mesh):
    return jax.shard_map(
        local,
        mesh=mesh,
        in_specs=(
            P(("dom", "sub"), None, None),
            P(("dom", "sub"), None),
            P(("dom", "sub")),
            P(("dom", "sub"), None),
            P(("dom", "sub"), None),
            P(None, ("dom", "sub")),
            P(("dom", "sub")),
            P("dom", None),
            P("dom"),
        ),
        out_specs=P(("dom", "sub"), None, None),
        check_vma=False,
    )
```

```python
import functools
import math

import jax
import jax.numpy as jnp
from jax import lax
from jax.experimental import pallas as pl
from jax.experimental.pallas import tpu as pltpu
from jax.sharding import PartitionSpec as P

CUR_BIN = 2
SOFT = 0.04
F32 = jnp.float32
BF16 = jnp.bfloat16
I32 = jnp.int32

BETA = 0.3
POLY = (
    0.000177460321,
    0.334470999,
    0.374323182,
    0.116028516,
    0.555240376,
    -0.510157925,
    0.129925288,
)
LEAD = POLY[6]
MONIC = tuple(c / LEAD for c in POLY[:6])
TAIL = 1.0 / (BETA * math.sqrt(math.pi) * LEAD)
DECAY = -math.log2(math.e) / (4.0 * BETA * BETA)
OUT_SCALE = BETA * BETA * LEAD

WIDTHS = (128, 144, 160, 192, 256)
KI = 2
VMEM = pltpu.VMEM
SMEM = pltpu.SMEM
SLOTS = 8


def vspec():
    return pl.BlockSpec(memory_space=VMEM)


def sspec():
    return pl.BlockSpec(memory_space=SMEM)


def hspec():
    return pl.BlockSpec(memory_space=pltpu.MemorySpace.HBM)


def nt_dot(a, b):
    return lax.dot_general(a, b, (((1,), (1,)), ((), ())), preferred_element_type=F32)


def split3(v):
    first = v.astype(BF16).astype(F32)
    rest = v - first
    second = rest.astype(BF16).astype(F32)
    return first, second, rest - second


def fetch(sources, buffers, sems):
    copies = [pltpu.make_async_copy(a, b, sems.at[k]) for k, (a, b) in enumerate(zip(sources, buffers))]
    for copy in copies:
        copy.start()
    return copies


def request_kernel(*refs):
    sources, (req_ref, slot_ref, nodes_ref), held, sems = refs[:5], refs[5:8], refs[8:13], refs[13]
    for copy in fetch(sources, held, sems):
        copy.wait()
    targets_ref, groups_ref, counts_ref, pos_ref, mass_ref = held
    most = targets_ref.shape[0]
    pairs = most * targets_ref.shape[1]
    domains = req_ref.shape[0]

    def in_line(ref):
        return jnp.concatenate([ref[v : v + 1, :] for v in range(most)], axis=1).astype(F32)

    dest = in_line(targets_ref)
    along = jnp.broadcast_to(dest, (pairs, pairs))
    down = jnp.transpose(along)
    earlier = lax.broadcasted_iota(I32, (pairs, pairs), 0) < lax.broadcasted_iota(I32, (pairs, pairs), 1)
    rank = jnp.sum(jnp.where((along == down) & earlier, 1.0, 0.0), axis=0, keepdims=True)
    slot = jnp.where(dest >= 0, dest * SLOTS + rank, -1.0)
    slot_ref[...] = slot.astype(I32)
    dom_id = lax.broadcasted_iota(I32, (domains, pairs), 0).astype(F32)
    asked = in_line(groups_ref) + 1.0
    by_dom = jnp.where(dom_id == dest, asked, 0.0).astype(BF16)
    lane_id = lax.broadcasted_iota(I32, (128, pairs), 0).astype(F32)
    by_rank = jnp.where(lane_id == rank, 1.0, 0.0).astype(BF16)
    wanted = nt_dot(by_dom, by_rank).astype(I32)
    half = counts_ref.shape[1]
    tail = jnp.concatenate([jnp.zeros((1, 128 - half), I32), counts_ref[...]], axis=1)
    lanes = lax.broadcasted_iota(I32, (domains, 128), 1)
    req_ref[...] = jnp.where(lanes < 128 - half, wanted, jnp.broadcast_to(tail, (domains, 128)))
    rows = nodes_ref.shape[2]
    for r in range(rows):
        for c in range(3):
            nodes_ref[0, c, r : r + 1, :] = pos_ref[c : c + 1, 128 * r : 128 * r + 128]
        nodes_ref[0, 3, r : r + 1, :] = mass_ref[0:1, 128 * r : 128 * r + 128]
    for c in range(4):
        tile = nodes_ref[0, c]
        for s in range(1, nodes_ref.shape[0]):
            nodes_ref[s, c] = tile


def list_kernel(nodes_ref, lists_hbm, counts_hbm, tab_ref, table_ref, lists_ref, counts_ref, one_ref, found_a, found_b, sems):
    sharers, _, rows, _ = nodes_ref.shape
    total = sharers * rows
    octets = lists_ref.shape[0] // 8
    found_refs = (found_a, found_b)
    copies = fetch((lists_hbm, counts_hbm), (lists_ref, counts_ref), sems)
    for c in range(3):
        tall = jnp.concatenate([nodes_ref[s, c] for s in range(sharers)], axis=0)
        parts = split3(jnp.transpose(tall) * BETA)
        for k in range(3):
            table_ref[128 * c : 128 * c + 128, total * k : total * k + total] = parts[k].astype(BF16)
    for copy in copies:
        copy.wait()
    row16 = lax.broadcasted_iota(I32, (16, 256), 0)
    row8 = lax.broadcasted_iota(I32, (8, 256), 0)
    entry_id = lax.broadcasted_iota(I32, (1, 256), 1)

    def gather(i, carry):
        first = pl.multiple_of(i * 8, 8)
        lane = [lists_ref[pl.ds(first, 8), 128 * h : 128 * h + 128] & 127 for h in range(2)]
        row = [lists_ref[pl.ds(first, 8), 128 * h : 128 * h + 128] >> 7 for h in range(2)]

        def search(k):
            at = jnp.broadcast_to(lists_ref[pl.ds(first + k, 1), :] >> 7, (16, 256))
            for j in range(total // 16):
                piece = jnp.where(row16 == at - 16 * j, 1.0, 0.0).astype(BF16)
                for part in range(3):
                    one_ref[k % 2, total * part + 16 * j : total * part + 16 * j + 16, :] = piece
            found_refs[k % 2][...] = jnp.dot(table_ref[...], one_ref[k % 2], preferred_element_type=F32)

        def select(k):
            at = jnp.broadcast_to(lists_ref[pl.ds(first + k, 1), :] & 127, (8, 256))
            valid = entry_id < counts_ref[first + k]
            sums = [jnp.zeros((8, 256), F32)] * 3
            for j in range(16):
                here = row8 == at - 8 * j
                for c in range(3):
                    piece = found_refs[k % 2][128 * c + 8 * j : 128 * c + 8 * j + 8, :]
                    sums[c] = sums[c] + jnp.where(here, piece, 0.0)
            for c in range(3):
                value = jnp.where(valid, jnp.sum(sums[c], axis=0, keepdims=True), 0.0)
                for h in range(2):
                    tab_ref[first + k, 4 * h + c : 4 * h + c + 1, :] = value[:, 128 * h : 128 * h + 128]

        masses = [jnp.zeros((8, 128), F32)] * 2
        for s in range(sharers):
            search(s)
            for r in range(rows):
                spread = jnp.broadcast_to(nodes_ref[s, 3, r : r + 1, :], (8, 128))
                for h in range(2):
                    picked = jnp.take_along_axis(spread, lane[h], axis=1, mode="promise_in_bounds")
                    masses[h] = jnp.where(row[h] == s * rows + r, picked, masses[h])
            if s > 0:
                select(s - 1)
        select(sharers - 1)
        for k in range(8):
            for h in range(2):
                keep = entry_id[:, 128 * h : 128 * h + 128] < counts_ref[first + k]
                tab_ref[first + k, 4 * h + 3 : 4 * h + 4, :] = jnp.where(keep, masses[h][k : k + 1, :], 0.0)
        return carry

    lax.fori_loop(0, octets, gather, 0)


def pack_kernel(req_ref, tab_ref, reply_ref):
    def pack(d, carry):
        for j in range(SLOTS):
            group = jnp.maximum(req_ref[d, j] - 1, 0)
            reply_ref[d, j] = tab_ref[group]
        return carry

    lax.fori_loop(0, reply_ref.shape[0], pack, 0)


def row_masks():
    row = lax.broadcasted_iota(I32, (8, 128), 0)
    return row < 4, row % 4 == 3, row


def list_features(tile):
    low, last, row = row_masks()
    sq = tile * tile
    norm = pltpu.roll(sq, 1, 0) + pltpu.roll(sq, 2, 0) + pltpu.roll(sq, 3, 0)
    g = split3(jnp.where(last, norm, tile))
    ga = [pltpu.roll(v, 4, 0) for v in g]

    def pair(a, b, h):
        if h == 0:
            return jnp.where(low, g[a], ga[b])
        return jnp.where(low, ga[a], g[b])

    ones = jnp.where(row < 3, 1.0, 0.0)
    feats = jnp.concatenate(
        [
            jnp.concatenate([pair(0, 0, h), pair(0, 1, h), pair(1, 2, h), ones], axis=0)
            for h in range(2)
        ],
        axis=1,
    ).astype(BF16)
    m1, m2, m3 = pltpu.roll(tile, 7, 0), pltpu.roll(tile, 6, 0), pltpu.roll(tile, 5, 0)
    col = row % 4
    mass = jnp.where(col == 0, m3, jnp.where(col == 1, m2, m1))
    w = split3(jnp.where(last, tile, tile * mass))
    wa = [pltpu.roll(v, 4, 0) for v in w]
    zero = jnp.zeros((8, 128), F32)
    loaded = jnp.concatenate(
        [
            jnp.concatenate(
                [
                    jnp.where(low, w[0], wa[1]) if h == 0 else jnp.where(low, wa[0], w[1]),
                    jnp.where(low, w[2] if h == 0 else wa[2], zero),
                ],
                axis=0,
            )
            for h in range(2)
        ],
        axis=1,
    ).astype(BF16)
    return feats, loaded


def weights(s):
    q = lax.rsqrt(s)
    t = 1.0 / (s * q + 1.0)
    p = t + MONIC[5]
    for k in (4, 3, 2, 1, 0):
        p = p * t + MONIC[k]
    e = jnp.exp2(s * DECAY)
    return (q * q) * e * (q * p + TAIL)


def run_items(groups, blk_ref, row_ref, nact_ref, fc_ref, tab_ref, acc_ref, bufs):
    last_block = fc_ref.shape[0] - 1
    s_bufs, w_bufs, y_bufs = bufs

    def items(g):
        return [(g + 1) * KI + k for k in range(KI)]

    def widest(g):
        n = I32(0)
        for i in items(g):
            n = jnp.maximum(n, nact_ref[jnp.minimum(blk_ref[i], last_block)])
        return n

    def prepare(g, par, width):
        for k, i in enumerate(items(g)):
            b = jnp.minimum(blk_ref[i], last_block)
            feats, loaded = list_features(tab_ref[row_ref[i]])
            y_bufs[par][k][...] = loaded
            wide = 128 if width == 128 else 256
            columns = jnp.transpose(fc_ref[b, :, :wide])[:width]
            s_bufs[par][k][:width, :] = jnp.dot(columns, feats, preferred_element_type=F32)

    def weigh(par, width):
        for j in range(0, width, 16):
            for k in range(KI):
                w = weights(s_bufs[par][k][j : j + 16, :])
                hi = w.astype(BF16)
                w_bufs[par][k][0, j : j + 16, :] = hi
                w_bufs[par][k][1, j : j + 16, :] = (w - hi.astype(F32)).astype(BF16)

    def reduce(g, par, width):
        made = []
        for k in range(KI):
            loaded = y_bufs[par][k][...]
            made.append(
                nt_dot(loaded, w_bufs[par][k][0, :width, :]) + nt_dot(loaded, w_bufs[par][k][1, :width, :])
            )
        return made

    def add(g, made, width):
        for k, i in enumerate(items(g)):
            b = blk_ref[i]
            acc_ref[b, :, :width] = acc_ref[b, :, :width] + made[k]

    def by_width(n, body):
        low = -1
        for width in WIDTHS:
            @pl.when((n > low) & (n <= width))
            def _(width=width):
                body(width)
            low = width

    def step(g, par):
        n = jnp.maximum(jnp.maximum(widest(g), widest(g + 1)), widest(g - 1))

        def body(width):
            made = reduce(g - 1, 1 - par, width)
            prepare(g + 1, 1 - par, width)
            weigh(par, width)
            add(g - 1, made, width)

        by_width(n, body)

    for k in range(KI):
        w_bufs[1][k][...] = jnp.zeros(w_bufs[1][k].shape, BF16)
        y_bufs[1][k][...] = jnp.zeros(y_bufs[1][k].shape, BF16)
    prepare(0, 0, 256)

    def pair(gg, carry):
        step(2 * gg, 0)
        step(2 * gg + 1, 1)
        return carry

    lax.fori_loop(0, (groups + 2) // 2, pair, 0)


def buffers():
    return (
        *[VMEM((256, 256), F32) for _ in range(2 * KI)],
        *[VMEM((2, 256, 256), BF16) for _ in range(2 * KI)],
        *[VMEM((16, 256), BF16) for _ in range(2 * KI)],
    )


def take_buffers(flat):
    n = 2 * KI
    return [[flat[j * n : j * n + KI], flat[j * n + KI : j * n + n]] for j in range(3)]


PAD = 6 * KI


def home_kernel(
    home_ref, slot_ref, nact_ref, pos_ref, bins_ref, tab_ref, fc_ref, key_ref, acc_ref, blk_out, row_out, n_out, blk_ref, row_ref, chosen_ref, *flat
):
    _, blocks, width = pos_ref.shape
    active = bins_ref[...] <= CUR_BIN
    tri = lax.broadcasted_iota(I32, (width, width), 0) <= lax.broadcasted_iota(I32, (width, width), 1)
    upto = jnp.dot(
        jnp.where(active, 1.0, 0.0).astype(BF16),
        jnp.where(tri, 1.0, 0.0).astype(BF16),
        preferred_element_type=F32,
    )
    key_ref[...] = jnp.where(active, upto - 1.0, -1.0).astype(I32)

    low8 = lax.broadcasted_iota(I32, (8, width), 0) < 4
    row8 = lax.broadcasted_iota(I32, (8, width), 0)
    row16 = lax.broadcasted_iota(I32, (16, width), 0)

    def compact(bb, carry):
        for u in range(4):
            b = bb * 4 + u
            key = jnp.broadcast_to(key_ref[pl.ds(b, 1), :], (16, width))
            for j in range(0, width, 16):
                chosen_ref[u, j : j + 16, :] = jnp.where(row16 == key - j, 1.0, 0.0).astype(BF16)
            pos = jnp.concatenate(
                [pos_ref[c, pl.ds(b, 1), :] * BETA for c in range(3)] + [jnp.zeros((5, width), F32)], axis=0
            )
            parts = jnp.concatenate(split3(pos), axis=0).astype(BF16)
            moved = nt_dot(parts, chosen_ref[u])
            x = (moved[0:8] + moved[8:16]) + moved[16:24]
            sq = x * x
            norm = sq[0:1] + sq[1:2] + sq[2:3] + SOFT * BETA * BETA
            n1, n2, n3 = split3(norm)
            a1, a2, a3 = split3(x * -2.0)
            unit = jnp.where(row8 == 3, 1.0, 0.0)
            a1 = a1 + unit
            r1, r2 = pltpu.roll(a1, 4, 0), pltpu.roll(a2, 4, 0)
            feats = jnp.concatenate(
                [
                    jnp.where(low8, a1, r2),
                    jnp.where(low8, a3, r1),
                    jnp.where(low8, a2, r1),
                    jnp.concatenate([n1, n2, n3, jnp.zeros((5, width), F32)], axis=0),
                ],
                axis=0,
            )
            fc_ref[b] = feats.astype(BF16)
            acc_ref[b] = jnp.zeros((16, width), F32)
        return carry

    lax.fori_loop(0, blocks // 4, compact, 0)
    acc_ref[blocks] = jnp.zeros((16, width), F32)

    def home_item(i, carry):
        inside = (i >= KI) & (i < blocks + KI)
        b = jnp.clip(i - KI, 0, blocks - 1)
        blk_ref[i] = jnp.where(inside, b, blocks)
        row_ref[i] = jnp.where(inside, home_ref[b], 0)
        return carry

    lax.fori_loop(0, blocks + PAD, home_item, 0)
    run_items(blocks // KI, blk_ref, row_ref, nact_ref, fc_ref, tab_ref, acc_ref, take_buffers(flat))

    most = slot_ref.shape[1] // blocks

    def no_item(k, carry):
        blk_out[k] = blocks
        row_out[k] = 0
        return carry

    lax.fori_loop(0, KI, no_item, 0)

    def visits(b, n):
        for v in range(most):
            slot = slot_ref[0, v * blocks + b]
            blk_out[n] = b
            row_out[n] = jnp.maximum(slot, 0)
            n = n + jnp.where(slot >= 0, 1, 0)
        return n

    end = lax.fori_loop(0, blocks, visits, I32(KI))
    lax.fori_loop(end, end + PAD - KI, no_item, 0)
    n_out[0] = end - KI


def remote_kernel(n_ref, blk_ref, row_ref, nact_ref, fc_ref, tab_ref, acc_in_ref, key_ref, pos_ref, out_ref, acc_ref, *flat):
    blocks = pos_ref.shape[1]
    acc_ref[...] = acc_in_ref[...]
    run_items((n_ref[0] + KI - 1) // KI, blk_ref, row_ref, nact_ref, fc_ref, tab_ref, acc_ref, take_buffers(flat))

    def finish(bb, carry):
        for u in range(4):
            b = bb * 4 + u
            acc = acc_ref[b]
            top = acc[0:8]
            total = top + pltpu.roll(top, 4, 0) + acc[8:16]
            key = key_ref[pl.ds(b, 1), :]
            parts = []
            for h in range(2):
                at = jnp.broadcast_to(key[:, 128 * h : 128 * h + 128], (8, 128))
                lane = at & 127
                left = jnp.take_along_axis(total[:, :128], lane, axis=1, mode="promise_in_bounds")
                right = jnp.take_along_axis(total[:, 128:], lane, axis=1, mode="promise_in_bounds")
                parts.append(jnp.where(at < 128, left, right))
            back = jnp.concatenate(parts, axis=1)
            for c in range(3):
                pull = (back[c : c + 1] - pos_ref[c, pl.ds(b, 1), :] * (BETA * back[3:4])) * OUT_SCALE
                out_ref[c, pl.ds(b, 1), :] = jnp.where(key >= 0, pull, 0.0)
        return carry

    lax.fori_loop(0, blocks // 4, finish, 0)


def local(positions, time_bins, home_groups, targets, target_groups, node_pos, node_mass, node_lists, list_counts):
    domains = lax.axis_size("dom")
    sharers = lax.axis_size("sub")
    blocks, most = targets.shape
    pairs = blocks * most
    width = positions.shape[2]
    lists = node_lists.shape[0]
    rows = node_mass.shape[0] // 128

    asked = (targets.T, target_groups.T, list_counts.reshape(1, lists), node_pos, node_mass.reshape(1, -1))
    req, slot, nodes = pl.pallas_call(
        request_kernel,
        out_shape=(
            jax.ShapeDtypeStruct((domains, 128), I32),
            jax.ShapeDtypeStruct((1, pairs), I32),
            jax.ShapeDtypeStruct((sharers, 4, rows, 128), F32),
        ),
        in_specs=[hspec()] * 5,
        out_specs=(vspec(),) * 3,
        scratch_shapes=[*[VMEM(a.shape, a.dtype) for a in asked], pltpu.SemaphoreType.DMA((5,))],
        compiler_params=pltpu.CompilerParams(vmem_limit_bytes=60 << 20),
        name="requests",
    )(*asked)
    nodes = lax.all_to_all(nodes, "sub", 0, 0, tiled=True)
    req = lax.all_to_all(req.reshape(domains, 1, 128), "dom", 0, 0, tiled=True).reshape(domains, 128)
    nact = jnp.sum((time_bins <= CUR_BIN).astype(I32), axis=1)

    tab = pl.pallas_call(
        list_kernel,
        out_shape=jax.ShapeDtypeStruct((lists, 8, 128), F32),
        in_specs=[vspec(), hspec(), hspec()],
        out_specs=vspec(),
        scratch_shapes=[
            VMEM((384, 3 * sharers * rows), BF16),
            VMEM(node_lists.shape, I32),
            SMEM(list_counts.shape, I32),
            VMEM((2, 3 * sharers * rows, 256), BF16),
            VMEM((384, 256), F32),
            VMEM((384, 256), F32),
            pltpu.SemaphoreType.DMA((2,)),
        ],
        compiler_params=pltpu.CompilerParams(vmem_limit_bytes=60 << 20),
        cost_estimate=pl.CostEstimate(flops=20_000_000, bytes_accessed=1_000_000, transcendentals=0),
        name="lists",
    )(nodes, node_lists, list_counts)

    reply = pl.pallas_call(
        pack_kernel,
        out_shape=jax.ShapeDtypeStruct((domains, SLOTS, 8, 128), F32),
        in_specs=[sspec(), vspec()],
        out_specs=vspec(),
        compiler_params=pltpu.CompilerParams(vmem_limit_bytes=60 << 20),
        name="pack",
    )(req, tab)
    reply = lax.all_to_all(reply.reshape(domains, SLOTS * 8, 128), "dom", 0, 0, tiled=True)

    positions = jnp.transpose(positions, (1, 0, 2))
    room = pairs + PAD
    fc, key, acc, blk, row, n = pl.pallas_call(
        home_kernel,
        out_shape=(
            jax.ShapeDtypeStruct((blocks, 32, width), BF16),
            jax.ShapeDtypeStruct((blocks, width), I32),
            jax.ShapeDtypeStruct((blocks + 1, 16, width), F32),
            jax.ShapeDtypeStruct((room,), I32),
            jax.ShapeDtypeStruct((room,), I32),
            jax.ShapeDtypeStruct((8,), I32),
        ),
        in_specs=[sspec(), sspec(), sspec(), vspec(), vspec(), vspec()],
        out_specs=(vspec(),) * 3 + (sspec(),) * 3,
        scratch_shapes=[SMEM((blocks + PAD,), I32), SMEM((blocks + PAD,), I32), VMEM((4, width, width), BF16), *buffers()],
        compiler_params=pltpu.CompilerParams(vmem_limit_bytes=60 << 20),
        cost_estimate=pl.CostEstimate(flops=40_000_000, bytes_accessed=4_000_000, transcendentals=12_000_000),
        name="home_pulls",
    )(home_groups, slot, nact, positions, time_bins, tab)

    out = pl.pallas_call(
        remote_kernel,
        out_shape=jax.ShapeDtypeStruct((3, blocks, width), F32),
        in_specs=[sspec()] * 4 + [vspec()] * 5,
        out_specs=vspec(),
        scratch_shapes=[VMEM((blocks + 1, 16, width), F32), *buffers()],
        compiler_params=pltpu.CompilerParams(vmem_limit_bytes=60 << 20),
        name="remote_pulls",
    )(n, blk, row, nact, fc, reply.reshape(domains * SLOTS, 8, 128), acc, key, positions)
    return jnp.transpose(out, (1, 0, 2))


def solution(mesh):
    return jax.shard_map(
        local,
        mesh=mesh,
        in_specs=(
            P(("dom", "sub"), None, None),
            P(("dom", "sub"), None),
            P(("dom", "sub")),
            P(("dom", "sub"), None),
            P(("dom", "sub"), None),
            P(None, ("dom", "sub")),
            P(("dom", "sub")),
            P("dom", None),
            P("dom"),
        ),
        out_specs=P(("dom", "sub"), None, None),
        check_vma=False,
    )
```

```python
import math

import jax
import jax.numpy as jnp
from jax import lax
from jax.experimental import pallas as pl
from jax.experimental.pallas import tpu as pltpu
from jax.sharding import PartitionSpec as P


CUR_BIN = 2
SOFT = 0.04
F32 = jnp.float32
BF16 = jnp.bfloat16
I32 = jnp.int32

BETA = 0.3
POLY = (
    0.000177460321,
    0.334470999,
    0.374323182,
    0.116028516,
    0.555240376,
    -0.510157925,
    0.129925288,
)
LEAD = POLY[6]
MONIC = tuple(c / LEAD for c in POLY[:6])
TAIL = 1.0 / (BETA * math.sqrt(math.pi) * LEAD)
DECAY = -math.log2(math.e) / (4.0 * BETA * BETA)
OUT_SCALE = BETA * BETA * LEAD

WIDTHS = (128, 144, 160, 192, 256)
KI = 6
VMEM = pltpu.VMEM
SMEM = pltpu.SMEM
SLOTS = 8


def vspec():
    return pl.BlockSpec(memory_space=VMEM)


def sspec():
    return pl.BlockSpec(memory_space=SMEM)


def hspec():
    return pl.BlockSpec(memory_space=pltpu.MemorySpace.HBM)


def nt_dot(a, b):
    return lax.dot_general(a, b, (((1,), (1,)), ((), ())), preferred_element_type=F32)


def split3(v):
    first = v.astype(BF16).astype(F32)
    rest = v - first
    second = rest.astype(BF16).astype(F32)
    return first, second, rest - second


def fetch(sources, buffers, sems):
    copies = [pltpu.make_async_copy(a, b, sems.at[k]) for k, (a, b) in enumerate(zip(sources, buffers))]
    for copy in copies:
        copy.start()
    return copies


def request_kernel(*refs):
    sources, (req_ref, slot_ref, nodes_ref), held, sems = refs[:5], refs[5:8], refs[8:13], refs[13]
    for copy in fetch(sources, held, sems):
        copy.wait()
    targets_ref, groups_ref, counts_ref, pos_ref, mass_ref = held
    most = targets_ref.shape[0]
    pairs = most * targets_ref.shape[1]
    domains = req_ref.shape[0]

    def in_line(ref):
        return jnp.concatenate([ref[v : v + 1, :] for v in range(most)], axis=1).astype(F32)

    dest = in_line(targets_ref)
    along = jnp.broadcast_to(dest, (pairs, pairs))
    down = jnp.transpose(along)
    earlier = lax.broadcasted_iota(I32, (pairs, pairs), 0) < lax.broadcasted_iota(I32, (pairs, pairs), 1)
    rank = jnp.sum(jnp.where((along == down) & earlier, 1.0, 0.0), axis=0, keepdims=True)
    slot = jnp.where(dest >= 0, dest * SLOTS + rank, -1.0)
    slot_ref[...] = slot.astype(I32)
    dom_id = lax.broadcasted_iota(I32, (domains, pairs), 0).astype(F32)
    asked = in_line(groups_ref) + 1.0
    by_dom = jnp.where(dom_id == dest, asked, 0.0).astype(BF16)
    lane_id = lax.broadcasted_iota(I32, (128, pairs), 0).astype(F32)
    by_rank = jnp.where(lane_id == rank, 1.0, 0.0).astype(BF16)
    wanted = nt_dot(by_dom, by_rank).astype(I32)
    half = counts_ref.shape[1]
    tail = jnp.concatenate([jnp.zeros((1, 128 - half), I32), counts_ref[...]], axis=1)
    lanes = lax.broadcasted_iota(I32, (domains, 128), 1)
    req_ref[...] = jnp.where(lanes < 128 - half, wanted, jnp.broadcast_to(tail, (domains, 128)))
    for r in range(nodes_ref.shape[1]):
        for c in range(3):
            nodes_ref[c, r : r + 1, :] = pos_ref[c : c + 1, 128 * r : 128 * r + 128]
        nodes_ref[3, r : r + 1, :] = mass_ref[0:1, 128 * r : 128 * r + 128]


def list_kernel(*refs):
    chips = len(refs) - 10
    node_refs = refs[:chips]
    lists_hbm, counts_hbm, tab_ref, table_ref, lists_ref, counts_ref, one_ref, *found_refs, sems = refs[chips:]
    _, rows, _ = node_refs[0].shape
    total = chips * rows
    octets = lists_ref.shape[0] // 8
    copies = fetch((lists_hbm, counts_hbm), (lists_ref, counts_ref), sems)
    sharers = lax.axis_size("sub")
    bases = [lax.rem(lax.axis_index("sub") + sharers - 2 * j, sharers) * rows for j in range(chips)]
    for c in range(3):
        tall = jnp.concatenate([ref[c] for ref in node_refs], axis=0)
        parts = split3(jnp.transpose(tall) * BETA)
        for k in range(3):
            table_ref[128 * c : 128 * c + 128, total * k : total * k + total] = parts[k].astype(BF16)
    for copy in copies:
        copy.wait()
    row16 = lax.broadcasted_iota(I32, (16, 256), 0)
    row8 = lax.broadcasted_iota(I32, (8, 256), 0)
    entry_id = lax.broadcasted_iota(I32, (1, 256), 1)

    def gather(i, carry):
        first = pl.multiple_of(i * 8, 8)
        lane = [lists_ref[pl.ds(first, 8), 128 * h : 128 * h + 128] & 127 for h in range(2)]
        row = [lists_ref[pl.ds(first, 8), 128 * h : 128 * h + 128] >> 7 for h in range(2)]

        def search(k):
            at = jnp.broadcast_to(lists_ref[pl.ds(first + k, 1), :] >> 7, (16, 256))
            for j in range(chips):
                for q in range(0, rows, 16):
                    piece = jnp.where(row16 == at - (bases[j] + q), 1.0, 0.0).astype(BF16)
                    for part in range(3):
                        put = total * part + rows * j + q
                        one_ref[k % 2, put : put + 16, :] = piece
            found_refs[k % 2][...] = jnp.dot(table_ref[...], one_ref[k % 2], preferred_element_type=F32)

        def select(k):
            at = jnp.broadcast_to(lists_ref[pl.ds(first + k, 1), :] & 127, (8, 256))
            valid = entry_id < counts_ref[first + k]
            sums = [jnp.zeros((8, 256), F32)] * 3
            for j in range(16):
                here = row8 == at - 8 * j
                for c in range(3):
                    piece = found_refs[k % 2][128 * c + 8 * j : 128 * c + 8 * j + 8, :]
                    sums[c] = sums[c] + jnp.where(here, piece, 0.0)
            for c in range(3):
                value = jnp.where(valid, jnp.sum(sums[c], axis=0, keepdims=True), 0.0)
                for h in range(2):
                    tab_ref[first + k, 4 * h + c : 4 * h + c + 1, :] = value[:, 128 * h : 128 * h + 128]

        masses = [jnp.zeros((8, 128), F32)] * 2
        step = rows * chips // 8
        for k in range(8):
            search(k)
            for r in range(k * step, k * step + step):
                j, inner = r // rows, r % rows
                spread = jnp.broadcast_to(node_refs[j][3, inner : inner + 1, :], (8, 128))
                for h in range(2):
                    picked = jnp.take_along_axis(spread, lane[h], axis=1, mode="promise_in_bounds")
                    masses[h] = jnp.where(row[h] == bases[j] + inner, picked, masses[h])
            if k > 0:
                select(k - 1)
        select(7)
        for k in range(8):
            for h in range(2):
                keep = entry_id[:, 128 * h : 128 * h + 128] < counts_ref[first + k]
                tab_ref[first + k, 4 * h + 3 : 4 * h + 4, :] = jnp.where(keep, masses[h][k : k + 1, :], 0.0)
        return carry

    lax.fori_loop(0, octets, gather, 0)


def build_lists(nodes, node_lists, list_counts):
    lists = node_lists.shape[0]
    deep = 3 * len(nodes) * nodes[0].shape[1]
    return pl.pallas_call(
        list_kernel,
        out_shape=jax.ShapeDtypeStruct((lists, 8, 128), F32),
        in_specs=[vspec()] * len(nodes) + [hspec(), hspec()],
        out_specs=vspec(),
        scratch_shapes=[
            VMEM((384, deep), BF16),
            VMEM(node_lists.shape, I32),
            SMEM(list_counts.shape, I32),
            VMEM((2, deep, 256), BF16),
            VMEM((384, 256), F32),
            VMEM((384, 256), F32),
            pltpu.SemaphoreType.DMA((2,)),
        ],
        compiler_params=pltpu.CompilerParams(vmem_limit_bytes=60 << 20),
        cost_estimate=pl.CostEstimate(flops=20_000_000, bytes_accessed=1_000_000, transcendentals=0),
        name="lists",
    )(*nodes, node_lists, list_counts)


def pack_kernel(req_ref, mine_ref, theirs_ref, tab_ref, reply_ref):
    tab_ref[...] = mine_ref[...] + theirs_ref[...]

    def pack(d, carry):
        for u in range(4):
            for j in range(SLOTS):
                group = jnp.maximum(req_ref[4 * d + u, j] - 1, 0)
                reply_ref[4 * d + u, j] = tab_ref[group]
        return carry

    lax.fori_loop(0, reply_ref.shape[0] // 4, pack, 0)


def row_masks():
    row = lax.broadcasted_iota(I32, (8, 128), 0)
    return row < 4, row % 4 == 3, row


def list_features(tile):
    low, last, row = row_masks()
    sq = tile * tile
    norm = pltpu.roll(sq, 1, 0) + pltpu.roll(sq, 2, 0) + pltpu.roll(sq, 3, 0)
    g = split3(jnp.where(last, norm, tile))
    ga = [pltpu.roll(v, 4, 0) for v in g]

    def pair(a, b, h):
        if h == 0:
            return jnp.where(low, g[a], ga[b])
        return jnp.where(low, ga[a], g[b])

    ones = jnp.where(row < 3, 1.0, 0.0)
    feats = jnp.concatenate(
        [
            jnp.concatenate([pair(0, 0, h), pair(0, 1, h), pair(1, 2, h), ones], axis=0)
            for h in range(2)
        ],
        axis=1,
    ).astype(BF16)
    m1, m2, m3 = pltpu.roll(tile, 7, 0), pltpu.roll(tile, 6, 0), pltpu.roll(tile, 5, 0)
    col = row % 4
    mass = jnp.where(col == 0, m3, jnp.where(col == 1, m2, m1))
    w = split3(jnp.where(last, tile, tile * mass))
    wa = [pltpu.roll(v, 4, 0) for v in w]
    zero = jnp.zeros((8, 128), F32)
    loaded = jnp.concatenate(
        [
            jnp.concatenate(
                [
                    jnp.where(low, w[0], wa[1]) if h == 0 else jnp.where(low, wa[0], w[1]),
                    jnp.where(low, w[2] if h == 0 else wa[2], zero),
                ],
                axis=0,
            )
            for h in range(2)
        ],
        axis=1,
    ).astype(BF16)
    return feats, loaded


def weights(s):
    q = lax.rsqrt(s)
    t = 1.0 / (s * q + 1.0)
    p = t + MONIC[5]
    for k in (4, 3, 2, 1, 0):
        p = p * t + MONIC[k]
    e = jnp.exp2(s * DECAY)
    return (q * q) * e * (q * p + TAIL)


def run_items(groups, blk_ref, half_ref, nact_ref, fc_ref, tab_ref, acc_ref, bufs):
    last_block = fc_ref.shape[0] - 1
    s_bufs, y_bufs = bufs

    def items(g):
        return [g * KI + k for k in range(KI)]

    def widest(g):
        n = I32(0)
        for i in items(g):
            n = jnp.maximum(n, nact_ref[jnp.minimum(blk_ref[i], last_block)])
        return n

    def two_halves(first, second):
        low, _, _ = row_masks()
        a = tab_ref[first >> 1]
        b = tab_ref[jnp.maximum(second, 0) >> 1]
        a = jnp.where((first & 1) == 1, pltpu.roll(a, 4, 0), a)
        b = jnp.where((second & 1) == 1, b, pltpu.roll(b, 4, 0))
        return jnp.where(low, a, jnp.where(second >= 0, b, 0.0))

    def prepare(g, k, width):
        i = g * KI + k
        b = jnp.minimum(blk_ref[i], last_block)
        feats, loaded = list_features(two_halves(half_ref[2 * i], half_ref[2 * i + 1]))
        y_bufs[k][...] = loaded
        wide = 128 if width == 128 else 256
        columns = jnp.transpose(fc_ref[b, :, :wide])[:width]
        s_bufs[k][:width, :] = jnp.dot(columns, feats, preferred_element_type=F32)

    def reduce(k, width):
        his, los = [], []
        for j in range(0, width, 16):
            w = weights(s_bufs[k][j : j + 16, :])
            hi = w.astype(BF16)
            his.append(hi)
            los.append((w - hi.astype(F32)).astype(BF16))
        loaded = y_bufs[k][...]
        return nt_dot(loaded, jnp.concatenate(his, axis=0)) + nt_dot(loaded, jnp.concatenate(los, axis=0))

    def by_width(n, body):
        low = -1
        for width in WIDTHS:
            @pl.when((n > low) & (n <= width))
            def _(width=width):
                body(width)

            low = width

    def step(g, carry):
        n = jnp.maximum(widest(g), widest(g + 1))

        def body(width):
            made = []
            for k in range(KI):
                made.append(reduce(k, width))
                prepare(g + 1, k, width)
            for k, i in enumerate(items(g)):
                b = blk_ref[i]
                acc_ref[b, :, :width] = acc_ref[b, :, :width] + made[k]

        by_width(n, body)
        return carry

    for k in range(KI):
        prepare(0, k, 256)
    lax.fori_loop(0, groups, step, 0)


def buffers():
    return (
        *[VMEM((256, 256), F32) for _ in range(KI)],
        *[VMEM((16, 256), BF16) for _ in range(KI)],
    )


def take_buffers(flat):
    return flat[:KI], flat[KI:]


PAD = 3 * KI


def home_kernel(
    home_ref, slot_ref, groups_ref, req_ref, nact_ref, pos_ref, bins_ref, tab_ref,
    fc_ref, key_ref, acc_ref, blk_out, half_out, n_out, blk_ref, half_ref, chosen_ref, *flat
):
    _, blocks, width = pos_ref.shape
    active = bins_ref[...] <= CUR_BIN
    tri = lax.broadcasted_iota(I32, (width, width), 0) <= lax.broadcasted_iota(I32, (width, width), 1)
    upto = jnp.dot(
        jnp.where(active, 1.0, 0.0).astype(BF16),
        jnp.where(tri, 1.0, 0.0).astype(BF16),
        preferred_element_type=F32,
    )
    key_ref[...] = jnp.where(active, upto - 1.0, -1.0).astype(I32)

    low8 = lax.broadcasted_iota(I32, (8, width), 0) < 4
    row8 = lax.broadcasted_iota(I32, (8, width), 0)
    row16 = lax.broadcasted_iota(I32, (16, width), 0)

    def compact(bb, carry):
        for u in range(4):
            b = bb * 4 + u
            key = jnp.broadcast_to(key_ref[pl.ds(b, 1), :], (16, width))
            for j in range(0, width, 16):
                chosen_ref[u, j : j + 16, :] = jnp.where(row16 == key - j, 1.0, 0.0).astype(BF16)
            pos = jnp.concatenate(
                [pos_ref[c, pl.ds(b, 1), :] * BETA for c in range(3)] + [jnp.zeros((5, width), F32)], axis=0
            )
            parts = jnp.concatenate(split3(pos), axis=0).astype(BF16)
            moved = nt_dot(parts, chosen_ref[u])
            x = (moved[0:8] + moved[8:16]) + moved[16:24]
            sq = x * x
            norm = sq[0:1] + sq[1:2] + sq[2:3] + SOFT * BETA * BETA
            n1, n2, n3 = split3(norm)
            a1, a2, a3 = split3(x * -2.0)
            unit = jnp.where(row8 == 3, 1.0, 0.0)
            a1 = a1 + unit
            r1, r2 = pltpu.roll(a1, 4, 0), pltpu.roll(a2, 4, 0)
            feats = jnp.concatenate(
                [
                    jnp.where(low8, a1, r2),
                    jnp.where(low8, a3, r1),
                    jnp.where(low8, a2, r1),
                    jnp.concatenate([n1, n2, n3, jnp.zeros((5, width), F32)], axis=0),
                ],
                axis=0,
            )
            fc_ref[b] = feats.astype(BF16)
            acc_ref[b] = jnp.zeros((16, width), F32)
        return carry

    lax.fori_loop(0, blocks // 4, compact, 0)
    acc_ref[blocks] = jnp.zeros((16, width), F32)

    def home_item(i, carry):
        inside = i < blocks
        b = jnp.minimum(i, blocks - 1)
        blk_ref[i] = jnp.where(inside, i, blocks)
        half_ref[2 * i] = 2 * home_ref[b]
        half_ref[2 * i + 1] = 2 * home_ref[b] + 1
        return carry

    lax.fori_loop(0, blocks + PAD, home_item, 0)
    run_items((blocks + KI - 1) // KI, blk_ref, half_ref, nact_ref, fc_ref, tab_ref, acc_ref, take_buffers(flat))

    most = slot_ref.shape[1] // blocks
    lists = 128 // 2

    def visits(b, n):
        for v in range(most):
            slot = slot_ref[0, v * blocks + b]
            used = jnp.where(slot >= 0, 1, 0)
            place = jnp.maximum(slot, 0)
            count = req_ref[place >> 3, lists + groups_ref[v, b]]
            blk_out[n >> 1] = b
            half_out[n] = 2 * place
            n = n + used
            blk_out[n >> 1] = b
            half_out[n] = 2 * place + 1
            n = n + jnp.where(count > 128, used, 0)
        half_out[n] = -1
        return n + (n & 1)

    end = lax.fori_loop(0, blocks, visits, I32(0)) >> 1

    def no_item(k, carry):
        blk_out[k] = blocks
        half_out[2 * k] = 0
        half_out[2 * k + 1] = -1
        return carry

    lax.fori_loop(end, end + PAD, no_item, 0)
    n_out[0] = end


def remote_kernel(n_ref, blk_ref, half_ref, nact_ref, fc_ref, tab_ref, acc_in_ref, key_ref, pos_ref, out_ref, acc_ref, *flat):
    blocks = pos_ref.shape[1]
    acc_ref[...] = acc_in_ref[...]
    run_items((n_ref[0] + KI - 1) // KI, blk_ref, half_ref, nact_ref, fc_ref, tab_ref, acc_ref, take_buffers(flat))

    def finish(bb, carry):
        for u in range(4):
            b = bb * 4 + u
            acc = acc_ref[b]
            top = acc[0:8]
            total = top + pltpu.roll(top, 4, 0) + acc[8:16]
            key = key_ref[pl.ds(b, 1), :]
            parts = []
            for h in range(2):
                at = jnp.broadcast_to(key[:, 128 * h : 128 * h + 128], (8, 128))
                lane = at & 127
                left = jnp.take_along_axis(total[:, :128], lane, axis=1, mode="promise_in_bounds")
                right = jnp.take_along_axis(total[:, 128:], lane, axis=1, mode="promise_in_bounds")
                parts.append(jnp.where(at < 128, left, right))
            back = jnp.concatenate(parts, axis=1)
            for c in range(3):
                pull = (back[c : c + 1] - pos_ref[c, pl.ds(b, 1), :] * (BETA * back[3:4])) * OUT_SCALE
                out_ref[c, pl.ds(b, 1), :] = jnp.where(key >= 0, pull, 0.0)
        return carry

    lax.fori_loop(0, blocks // 4, finish, 0)


def forces_of(positions, time_bins, home_groups, targets, target_groups, node_pos, node_mass, node_lists, list_counts):
    domains = lax.axis_size("dom")
    sharers = lax.axis_size("sub")
    blocks, most = targets.shape
    pairs = blocks * most
    width = positions.shape[2]
    lists = node_lists.shape[0]
    rows = node_mass.shape[0] // 128

    asked = (targets.T, target_groups.T, list_counts.reshape(1, lists), node_pos, node_mass.reshape(1, -1))
    req, slot, nodes = pl.pallas_call(
        request_kernel,
        out_shape=(
            jax.ShapeDtypeStruct((domains, 128), I32),
            jax.ShapeDtypeStruct((1, pairs), I32),
            jax.ShapeDtypeStruct((4, rows, 128), F32),
        ),
        in_specs=[hspec()] * 5,
        out_specs=(vspec(),) * 3,
        scratch_shapes=[*[VMEM(a.shape, a.dtype) for a in asked], pltpu.SemaphoreType.DMA((5,))],
        compiler_params=pltpu.CompilerParams(vmem_limit_bytes=60 << 20),
        name="requests",
    )(*asked)
    held = [nodes]
    for j in range(1, sharers // 2):
        held.append(lax.ppermute(nodes, "sub", [(i, (i + 2 * j) % sharers) for i in range(sharers)]))
    req = lax.all_to_all(req.reshape(domains, 1, 128), "dom", 0, 0, tiled=True)
    req = req.reshape(domains, 128)
    nact = jnp.sum((time_bins <= CUR_BIN).astype(I32), axis=1)

    mine = build_lists(held, node_lists, list_counts)
    theirs = lax.ppermute(mine, "sub", [(i, i ^ 1) for i in range(sharers)])
    tab, reply = pl.pallas_call(
        pack_kernel,
        out_shape=(
            jax.ShapeDtypeStruct((lists, 8, 128), F32),
            jax.ShapeDtypeStruct((domains, SLOTS, 8, 128), F32),
        ),
        in_specs=[sspec(), vspec(), vspec()],
        out_specs=(vspec(),) * 2,
        compiler_params=pltpu.CompilerParams(vmem_limit_bytes=60 << 20),
        name="pack",
    )(req, mine, theirs)
    reply = lax.all_to_all(reply.reshape(domains, SLOTS * 8, 128), "dom", 0, 0, tiled=True)

    positions = jnp.transpose(positions, (1, 0, 2))
    room = pairs + PAD
    fc, key, acc, blk, half, n = pl.pallas_call(
        home_kernel,
        out_shape=(
            jax.ShapeDtypeStruct((blocks, 32, width), BF16),
            jax.ShapeDtypeStruct((blocks, width), I32),
            jax.ShapeDtypeStruct((blocks + 1, 16, width), F32),
            jax.ShapeDtypeStruct((room,), I32),
            jax.ShapeDtypeStruct((2 * room,), I32),
            jax.ShapeDtypeStruct((8,), I32),
        ),
        in_specs=[sspec()] * 5 + [vspec()] * 3,
        out_specs=(vspec(),) * 3 + (sspec(),) * 3,
        scratch_shapes=[SMEM((blocks + PAD,), I32), SMEM((2 * (blocks + PAD),), I32), VMEM((4, width, width), BF16), *buffers()],
        compiler_params=pltpu.CompilerParams(vmem_limit_bytes=60 << 20),
        cost_estimate=pl.CostEstimate(flops=40_000_000, bytes_accessed=4_000_000, transcendentals=12_000_000),
        name="home_pulls",
    )(home_groups, slot, target_groups.T, req, nact, positions, time_bins, tab)

    out = pl.pallas_call(
        remote_kernel,
        out_shape=jax.ShapeDtypeStruct((3, blocks, width), F32),
        in_specs=[sspec()] * 4 + [vspec()] * 5,
        out_specs=vspec(),
        scratch_shapes=[VMEM((blocks + 1, 16, width), F32), *buffers()],
        compiler_params=pltpu.CompilerParams(vmem_limit_bytes=60 << 20),
        name="remote_pulls",
    )(n, blk, half, nact, fc, reply.reshape(domains * SLOTS, 8, 128), acc, key, positions)
    return jnp.transpose(out, (1, 0, 2))


def solution(mesh):
    return jax.shard_map(
        forces_of,
        mesh=mesh,
        in_specs=(
            P(("dom", "sub"), None, None),
            P(("dom", "sub"), None),
            P(("dom", "sub")),
            P(("dom", "sub"), None),
            P(("dom", "sub"), None),
            P(None, ("dom", "sub")),
            P(("dom", "sub")),
            P("dom", None),
            P("dom"),
        ),
        out_specs=P(("dom", "sub"), None, None),
        check_vma=False,
    )
```

```python
import math

import jax
import jax.numpy as jnp
from jax import lax
from jax.experimental import pallas as pl
from jax.experimental.pallas import tpu as pltpu
from jax.sharding import PartitionSpec as P


CUR_BIN = 2
SOFT = 0.04
F32 = jnp.float32
BF16 = jnp.bfloat16
I32 = jnp.int32

SHIFT = 0.245
POLY = (
    0.999994348,
    -0.564111497,
    0.111462021,
    -0.00487730517,
    -0.00155512244,
    0.000185247258,
)
LEAD = POLY[5]
MONIC = tuple(c / LEAD for c in POLY[:5])
TAIL = 1.0 / (math.sqrt(math.pi) * LEAD)
DECAY = -0.25 * math.log2(math.e)

WIDTHS = (128, 144, 160, 192, 256)
KI = 6
VMEM = pltpu.VMEM
SMEM = pltpu.SMEM
SLOTS = 8


def vspec():
    return pl.BlockSpec(memory_space=VMEM)


def sspec():
    return pl.BlockSpec(memory_space=SMEM)


def hspec():
    return pl.BlockSpec(memory_space=pltpu.MemorySpace.HBM)


def nt_dot(a, b):
    return lax.dot_general(a, b, (((1,), (1,)), ((), ())), preferred_element_type=F32)


def split3(v):
    first = v.astype(BF16).astype(F32)
    rest = v - first
    second = rest.astype(BF16).astype(F32)
    return first, second, rest - second


def fetch(sources, buffers, sems):
    copies = [pltpu.make_async_copy(a, b, sems.at[k]) for k, (a, b) in enumerate(zip(sources, buffers))]
    for copy in copies:
        copy.start()
    return copies


def request_kernel(*refs):
    sources, (req_ref, slot_ref, nact_ref, nodes_ref), held, sems = refs[:6], refs[6:10], refs[10:16], refs[16]
    for copy in fetch(sources, held, sems):
        copy.wait()
    targets_ref, groups_ref, counts_ref, pos_ref, mass_ref, bins_ref = held
    most = targets_ref.shape[0]
    pairs = most * targets_ref.shape[1]
    domains = req_ref.shape[0]

    def in_line(ref):
        return jnp.concatenate([ref[v : v + 1, :] for v in range(most)], axis=1).astype(F32)

    dest = in_line(targets_ref)
    along = jnp.broadcast_to(dest, (pairs, pairs))
    down = jnp.transpose(along)
    earlier = lax.broadcasted_iota(I32, (pairs, pairs), 0) < lax.broadcasted_iota(I32, (pairs, pairs), 1)
    rank = jnp.sum(jnp.where((along == down) & earlier, 1.0, 0.0), axis=0, keepdims=True)
    slot = jnp.where(dest >= 0, dest * SLOTS + rank, -1.0)
    slot_ref[...] = slot.astype(I32)
    active = jnp.where(bins_ref[...] <= CUR_BIN, 1.0, 0.0).astype(BF16)
    nact_ref[...] = nt_dot(jnp.ones((16, active.shape[1]), BF16), active)[0:1].astype(I32)
    dom_id = lax.broadcasted_iota(I32, (domains, pairs), 0).astype(F32)
    asked = in_line(groups_ref) + 1.0
    by_dom = jnp.where(dom_id == dest, asked, 0.0).astype(BF16)
    lane_id = lax.broadcasted_iota(I32, (128, pairs), 0).astype(F32)
    by_rank = jnp.where(lane_id == rank, 1.0, 0.0).astype(BF16)
    wanted = nt_dot(by_dom, by_rank).astype(I32)
    half = counts_ref.shape[1]
    tail = jnp.concatenate([jnp.zeros((1, 128 - half), I32), counts_ref[...]], axis=1)
    lanes = lax.broadcasted_iota(I32, (domains, 128), 1)
    req_ref[...] = jnp.where(lanes < 128 - half, wanted, jnp.broadcast_to(tail, (domains, 128)))
    for r in range(nodes_ref.shape[1]):
        for c in range(3):
            nodes_ref[c, r : r + 1, :] = pos_ref[c : c + 1, 128 * r : 128 * r + 128]
        nodes_ref[3, r : r + 1, :] = mass_ref[0:1, 128 * r : 128 * r + 128]


def list_kernel(*refs):
    chips = len(refs) - 10
    node_refs = refs[:chips]
    lists_hbm, counts_hbm, tab_ref, table_ref, lists_ref, counts_ref, one_ref, *found_refs, sems = refs[chips:]
    _, rows, _ = node_refs[0].shape
    total = chips * rows
    octets = lists_ref.shape[0] // 8
    copies = fetch((lists_hbm, counts_hbm), (lists_ref, counts_ref), sems)
    sharers = lax.axis_size("sub")
    bases = [lax.rem(lax.axis_index("sub") + sharers - 2 * j, sharers) * rows for j in range(chips)]
    for c in range(3):
        tall = jnp.concatenate([ref[c] for ref in node_refs], axis=0)
        parts = split3(jnp.transpose(tall))
        for k in range(3):
            table_ref[128 * c : 128 * c + 128, total * k : total * k + total] = parts[k].astype(BF16)
    for copy in copies:
        copy.wait()
    row16 = lax.broadcasted_iota(I32, (16, 256), 0)
    row8 = lax.broadcasted_iota(I32, (8, 256), 0)
    entry_id = lax.broadcasted_iota(I32, (1, 256), 1)

    def gather(i, carry):
        first = pl.multiple_of(i * 8, 8)
        lane = [lists_ref[pl.ds(first, 8), 128 * h : 128 * h + 128] & 127 for h in range(2)]
        row = [lists_ref[pl.ds(first, 8), 128 * h : 128 * h + 128] >> 7 for h in range(2)]

        def search(k):
            at = jnp.broadcast_to(lists_ref[pl.ds(first + k, 1), :] >> 7, (16, 256))
            for j in range(chips):
                for q in range(0, rows, 16):
                    piece = jnp.where(row16 == at - (bases[j] + q), 1.0, 0.0).astype(BF16)
                    for part in range(3):
                        put = total * part + rows * j + q
                        one_ref[k % 2, put : put + 16, :] = piece
            found_refs[k % 2][...] = jnp.dot(table_ref[...], one_ref[k % 2], preferred_element_type=F32)

        def select(k):
            at = jnp.broadcast_to(lists_ref[pl.ds(first + k, 1), :] & 127, (8, 256))
            valid = entry_id < counts_ref[first + k]
            sums = [jnp.zeros((8, 256), F32)] * 3
            for j in range(16):
                here = row8 == at - 8 * j
                for c in range(3):
                    piece = found_refs[k % 2][128 * c + 8 * j : 128 * c + 8 * j + 8, :]
                    sums[c] = sums[c] + jnp.where(here, piece, 0.0)
            for c in range(3):
                value = jnp.where(valid, jnp.sum(sums[c], axis=0, keepdims=True), 0.0)
                for h in range(2):
                    tab_ref[first + k, 4 * h + c : 4 * h + c + 1, :] = value[:, 128 * h : 128 * h + 128]

        masses = [jnp.zeros((8, 128), F32)] * 2
        step = rows * chips // 8
        for k in range(8):
            search(k)
            for r in range(k * step, k * step + step):
                j, inner = r // rows, r % rows
                spread = jnp.broadcast_to(node_refs[j][3, inner : inner + 1, :], (8, 128))
                for h in range(2):
                    picked = jnp.take_along_axis(spread, lane[h], axis=1, mode="promise_in_bounds")
                    masses[h] = jnp.where(row[h] == bases[j] + inner, picked, masses[h])
            if k > 0:
                select(k - 1)
        select(7)
        for k in range(8):
            for h in range(2):
                keep = entry_id[:, 128 * h : 128 * h + 128] < counts_ref[first + k]
                tab_ref[first + k, 4 * h + 3 : 4 * h + 4, :] = jnp.where(keep, masses[h][k : k + 1, :], 0.0)
        return carry

    lax.fori_loop(0, octets, gather, 0)


def build_lists(nodes, node_lists, list_counts):
    lists = node_lists.shape[0]
    deep = 3 * len(nodes) * nodes[0].shape[1]
    return pl.pallas_call(
        list_kernel,
        out_shape=jax.ShapeDtypeStruct((lists, 8, 128), F32),
        in_specs=[vspec()] * len(nodes) + [hspec(), hspec()],
        out_specs=vspec(),
        scratch_shapes=[
            VMEM((384, deep), BF16),
            VMEM(node_lists.shape, I32),
            SMEM(list_counts.shape, I32),
            VMEM((2, deep, 256), BF16),
            VMEM((384, 256), F32),
            VMEM((384, 256), F32),
            pltpu.SemaphoreType.DMA((2,)),
        ],
        compiler_params=pltpu.CompilerParams(vmem_limit_bytes=60 << 20),
        cost_estimate=pl.CostEstimate(flops=20_000_000, bytes_accessed=1_000_000, transcendentals=0),
        name="lists",
    )(*nodes, node_lists, list_counts)


def pack_kernel(req_ref, mine_ref, theirs_ref, tab_ref, reply_ref):
    tab_ref[...] = mine_ref[...] + theirs_ref[...]

    def pack(d, carry):
        for u in range(4):
            for j in range(SLOTS):
                group = jnp.maximum(req_ref[4 * d + u, j] - 1, 0)
                reply_ref[4 * d + u, j] = tab_ref[group]
        return carry

    lax.fori_loop(0, reply_ref.shape[0] // 4, pack, 0)


def row_masks():
    row = lax.broadcasted_iota(I32, (8, 128), 0)
    return row < 4, row % 4 == 3, row


def list_features(tile):
    low, last, row = row_masks()
    sq = tile * tile
    norm = pltpu.roll(sq, 1, 0) + pltpu.roll(sq, 2, 0) + pltpu.roll(sq, 3, 0)
    g = split3(jnp.where(last, norm, tile))
    ga = [pltpu.roll(v, 4, 0) for v in g]

    def pair(a, b, h):
        if h == 0:
            return jnp.where(low, g[a], ga[b])
        return jnp.where(low, ga[a], g[b])

    ones = jnp.where(row < 3, 1.0, 0.0)
    feats = jnp.concatenate(
        [
            jnp.concatenate([pair(0, 0, h), pair(0, 1, h), pair(1, 2, h), ones], axis=0)
            for h in range(2)
        ],
        axis=1,
    ).astype(BF16)
    m1, m2, m3 = pltpu.roll(tile, 7, 0), pltpu.roll(tile, 6, 0), pltpu.roll(tile, 5, 0)
    col = row % 4
    mass = jnp.where(col == 0, m3, jnp.where(col == 1, m2, m1))
    w = split3(jnp.where(last, tile, tile * mass))
    wa = [pltpu.roll(v, 4, 0) for v in w]
    zero = jnp.zeros((8, 128), F32)
    loaded = jnp.concatenate(
        [
            jnp.concatenate(
                [
                    jnp.where(low, w[0], wa[1]) if h == 0 else jnp.where(low, wa[0], w[1]),
                    jnp.where(low, w[2] if h == 0 else wa[2], zero),
                ],
                axis=0,
            )
            for h in range(2)
        ],
        axis=1,
    ).astype(BF16)
    return feats, loaded


def weights(s):
    q = lax.rsqrt(s)
    t = 1.0 / (q + SHIFT)
    p = t + MONIC[4]
    for k in (3, 2, 1, 0):
        p = p * t + MONIC[k]
    e = jnp.exp2(s * DECAY)
    return (q * q) * e * (q * p + TAIL)


def run_items(groups, blk_ref, half_ref, nact_ref, fc_ref, tab_ref, acc_ref, bufs):
    last_block = fc_ref.shape[0] - 1
    nobody = acc_ref.shape[0] - 1
    s_bufs, y_bufs, w_buf = bufs
    last = KI - 1

    def active_in(i):
        return nact_ref[jnp.minimum(blk_ref[i], last_block)]

    def two_halves(first, second):
        low, _, _ = row_masks()
        a = tab_ref[first >> 1]
        b = tab_ref[jnp.maximum(second, 0) >> 1]
        a = jnp.where((first & 1) == 1, pltpu.roll(a, 4, 0), a)
        b = jnp.where((second & 1) == 1, b, pltpu.roll(b, 4, 0))
        return jnp.where(low, a, jnp.where(second >= 0, b, 0.0))

    def prepare(g, k, par, width):
        i = g * KI + k
        b = jnp.minimum(blk_ref[i], last_block)
        feats, loaded = list_features(two_halves(half_ref[2 * i], half_ref[2 * i + 1]))
        y_bufs[par][k][...] = loaded
        wide = 128 if width == 128 else 256
        columns = jnp.transpose(fc_ref[b, :, :wide])[:width]
        s_bufs[par][k][:width, :] = jnp.dot(columns, feats, preferred_element_type=F32)

    def split_weights(k, par, width):
        for j in range(0, width, 16):
            w = weights(s_bufs[par][k][j : j + 16, :])
            hi = w.astype(BF16)
            yield j, hi, (w - hi.astype(F32)).astype(BF16)

    def reduce(k, par, width):
        pieces = list(split_weights(k, par, width))
        loaded = y_bufs[par][k][...]
        hi = jnp.concatenate([p[1] for p in pieces], axis=0)
        lo = jnp.concatenate([p[2] for p in pieces], axis=0)
        return nt_dot(loaded, hi) + nt_dot(loaded, lo)

    def leave(par, width):
        for j, hi, lo in split_weights(last, par, width):
            w_buf[0, j : j + 16, :] = hi
            w_buf[1, j : j + 16, :] = lo

    def left(par, width):
        loaded = y_bufs[par][last][...]
        return nt_dot(loaded, w_buf[0, :width, :]) + nt_dot(loaded, w_buf[1, :width, :])

    def add(b, made, width):
        acc_ref[b, :, :width] = acc_ref[b, :, :width] + made

    def before(g):
        return jnp.where(g > 0, blk_ref[jnp.maximum(g * KI - 1, 0)], nobody)

    def by_width(n, body):
        low = -1
        for width in WIDTHS:
            @pl.when((n > low) & (n <= width))
            def _(width=width):
                body(width)

            low = width

    def step(g, par):
        n = nact_ref[jnp.minimum(before(g), last_block)]
        for k in range(2 * KI):
            n = jnp.maximum(n, active_in(g * KI + k))

        def body(width):
            old = left(1 - par, width)
            made = []
            for k in range(KI):
                prepare(g + 1, k, 1 - par, width)
            for k in range(KI):
                if k < last:
                    made.append(reduce(k, par, width))
                else:
                    leave(par, width)
            add(before(g), old, width)
            for k in range(last):
                add(blk_ref[g * KI + k], made[k], width)

        by_width(n, body)

    def two_steps(gg, carry):
        step(2 * gg, 0)
        step(2 * gg + 1, 1)
        return carry

    w_buf[...] = jnp.zeros(w_buf.shape, BF16)
    y_bufs[1][last][...] = jnp.zeros(y_bufs[1][last].shape, BF16)
    for k in range(KI):
        prepare(0, k, 0, 256)
    lax.fori_loop(0, (groups + 1) // 2, two_steps, 0)
    add(before(2 * ((groups + 1) // 2)), left(1, 256), 256)


def buffers():
    return (
        *[VMEM((256, 256), F32) for _ in range(2 * KI)],
        *[VMEM((16, 256), BF16) for _ in range(2 * KI)],
        VMEM((2, 256, 256), BF16),
    )


def take_buffers(flat):
    s, y = flat[: 2 * KI], flat[2 * KI : -1]
    return (s[:KI], s[KI:]), (y[:KI], y[KI:]), flat[-1]


PAD = 4 * KI


def home_kernel(
    home_ref, slot_ref, groups_ref, req_ref, nact_ref, pos_ref, bins_ref, tab_ref,
    fc_ref, key_ref, acc_ref, blk_out, half_out, n_out, blk_ref, half_ref, order_ref, chosen_ref, *flat
):
    _, blocks, width = pos_ref.shape
    active = bins_ref[...] <= CUR_BIN
    tri = lax.broadcasted_iota(I32, (width, width), 0) <= lax.broadcasted_iota(I32, (width, width), 1)
    upto = jnp.dot(
        jnp.where(active, 1.0, 0.0).astype(BF16),
        jnp.where(tri, 1.0, 0.0).astype(BF16),
        preferred_element_type=F32,
    )
    key_ref[...] = jnp.where(active, upto - 1.0, -1.0).astype(I32)

    low8 = lax.broadcasted_iota(I32, (8, width), 0) < 4
    row8 = lax.broadcasted_iota(I32, (8, width), 0)
    row16 = lax.broadcasted_iota(I32, (16, width), 0)

    def compact(bb, carry):
        for u in range(4):
            b = bb * 4 + u
            key = jnp.broadcast_to(key_ref[pl.ds(b, 1), :], (16, width))
            for j in range(0, width, 16):
                chosen_ref[u, j : j + 16, :] = jnp.where(row16 == key - j, 1.0, 0.0).astype(BF16)
            pos = jnp.concatenate(
                [pos_ref[c, pl.ds(b, 1), :] for c in range(3)] + [jnp.zeros((5, width), F32)], axis=0
            )
            parts = jnp.concatenate(split3(pos), axis=0).astype(BF16)
            moved = nt_dot(parts, chosen_ref[u])
            x = (moved[0:8] + moved[8:16]) + moved[16:24]
            sq = x * x
            norm = sq[0:1] + sq[1:2] + sq[2:3] + SOFT
            n1, n2, n3 = split3(norm)
            a1, a2, a3 = split3(x * -2.0)
            unit = jnp.where(row8 == 3, 1.0, 0.0)
            a1 = a1 + unit
            r1, r2 = pltpu.roll(a1, 4, 0), pltpu.roll(a2, 4, 0)
            feats = jnp.concatenate(
                [
                    jnp.where(low8, a1, r2),
                    jnp.where(low8, a3, r1),
                    jnp.where(low8, a2, r1),
                    jnp.concatenate([n1, n2, n3, jnp.zeros((5, width), F32)], axis=0),
                ],
                axis=0,
            )
            fc_ref[b] = feats.astype(BF16)
            acc_ref[b] = jnp.zeros((16, width), F32)
        return carry

    lax.fori_loop(0, blocks // 4, compact, 0)
    acc_ref[blocks] = jnp.zeros((16, width), F32)

    def home_item(i, carry):
        inside = i < blocks
        b = jnp.minimum(i, blocks - 1)
        blk_ref[i] = jnp.where(inside, i, blocks)
        half_ref[2 * i] = 2 * home_ref[b]
        half_ref[2 * i + 1] = 2 * home_ref[b] + 1
        return carry

    lax.fori_loop(0, blocks + PAD, home_item, 0)
    run_items((blocks + KI - 1) // KI, blk_ref, half_ref, nact_ref, fc_ref, tab_ref, acc_ref, take_buffers(flat))

    most = slot_ref.shape[1] // blocks
    lists = 128 // 2

    where = I32(0)
    low = -1
    for high in (WIDTHS[0], WIDTHS[1], WIDTHS[-1]):

        def place_block(b, n, low=low, high=high):
            order_ref[n] = b
            return n + jnp.where((nact_ref[b] > low) & (nact_ref[b] <= high), 1, 0)

        where = lax.fori_loop(0, blocks, place_block, where)
        low = high

    def visits(at, n):
        b = order_ref[at]
        for v in range(most):
            slot = slot_ref[0, v * blocks + b]
            used = jnp.where(slot >= 0, 1, 0)
            place = jnp.maximum(slot, 0)
            count = req_ref[place >> 3, lists + groups_ref[v, b]]
            blk_out[n >> 1] = b
            half_out[n] = 2 * place
            n = n + used
            blk_out[n >> 1] = b
            half_out[n] = 2 * place + 1
            n = n + jnp.where(count > 128, used, 0)
        half_out[n] = -1
        return n + (n & 1)

    end = lax.fori_loop(0, blocks, visits, I32(0)) >> 1

    def no_item(k, carry):
        blk_out[k] = blocks
        half_out[2 * k] = 0
        half_out[2 * k + 1] = -1
        return carry

    lax.fori_loop(end, end + PAD, no_item, 0)
    n_out[0] = end


def remote_kernel(n_ref, blk_ref, half_ref, nact_ref, fc_ref, tab_ref, acc_in_ref, key_ref, pos_ref, out_ref, acc_ref, *flat):
    blocks = pos_ref.shape[1]
    pltpu.sync_copy(acc_in_ref, acc_ref)
    run_items((n_ref[0] + KI - 1) // KI, blk_ref, half_ref, nact_ref, fc_ref, tab_ref, acc_ref, take_buffers(flat))

    def finish(bb, carry):
        for u in range(4):
            b = bb * 4 + u
            acc = acc_ref[b]
            top = acc[0:8]
            total = top + pltpu.roll(top, 4, 0) + acc[8:16]
            key = key_ref[pl.ds(b, 1), :]
            parts = []
            for h in range(2):
                at = jnp.broadcast_to(key[:, 128 * h : 128 * h + 128], (8, 128))
                lane = at & 127
                left = jnp.take_along_axis(total[:, :128], lane, axis=1, mode="promise_in_bounds")
                right = jnp.take_along_axis(total[:, 128:], lane, axis=1, mode="promise_in_bounds")
                parts.append(jnp.where(at < 128, left, right))
            back = jnp.concatenate(parts, axis=1)
            for c in range(3):
                pull = (back[c : c + 1] - pos_ref[c, pl.ds(b, 1), :] * back[3:4]) * LEAD
                out_ref[c, pl.ds(b, 1), :] = jnp.where(key >= 0, pull, 0.0)
        return carry

    lax.fori_loop(0, blocks // 4, finish, 0)


def forces_of(positions, time_bins, home_groups, targets, target_groups, node_pos, node_mass, node_lists, list_counts):
    domains = lax.axis_size("dom")
    sharers = lax.axis_size("sub")
    blocks, most = targets.shape
    pairs = blocks * most
    width = positions.shape[2]
    lists = node_lists.shape[0]
    rows = node_mass.shape[0] // 128

    asked = (targets.T, target_groups.T, list_counts.reshape(1, lists), node_pos, node_mass.reshape(1, -1), time_bins)
    req, slot, nact, nodes = pl.pallas_call(
        request_kernel,
        out_shape=(
            jax.ShapeDtypeStruct((domains, 128), I32),
            jax.ShapeDtypeStruct((1, pairs), I32),
            jax.ShapeDtypeStruct((1, blocks), I32),
            jax.ShapeDtypeStruct((4, rows, 128), F32),
        ),
        in_specs=[hspec()] * 6,
        out_specs=(vspec(),) * 4,
        scratch_shapes=[*[VMEM(a.shape, a.dtype) for a in asked], pltpu.SemaphoreType.DMA((6,))],
        compiler_params=pltpu.CompilerParams(vmem_limit_bytes=60 << 20),
        name="requests",
    )(*asked)
    held = [nodes]
    for j in range(1, sharers // 2):
        held.append(lax.ppermute(nodes, "sub", [(i, (i + 2 * j) % sharers) for i in range(sharers)]))
    req = lax.all_to_all(req.reshape(domains, 1, 128), "dom", 0, 0, tiled=True)
    req = req.reshape(domains, 128)
    nact = nact.reshape(blocks)

    mine = build_lists(held, node_lists, list_counts)
    theirs = lax.ppermute(mine, "sub", [(i, i ^ 1) for i in range(sharers)])
    tab, reply = pl.pallas_call(
        pack_kernel,
        out_shape=(
            jax.ShapeDtypeStruct((lists, 8, 128), F32),
            jax.ShapeDtypeStruct((domains, SLOTS, 8, 128), F32),
        ),
        in_specs=[sspec(), vspec(), vspec()],
        out_specs=(vspec(),) * 2,
        compiler_params=pltpu.CompilerParams(vmem_limit_bytes=60 << 20),
        name="pack",
    )(req, mine, theirs)
    reply = lax.all_to_all(reply.reshape(domains, SLOTS * 8, 128), "dom", 0, 0, tiled=True)

    positions = jnp.transpose(positions, (1, 0, 2))
    room = pairs + PAD
    fc, key, acc, blk, half, n = pl.pallas_call(
        home_kernel,
        out_shape=(
            jax.ShapeDtypeStruct((blocks, 32, width), BF16),
            jax.ShapeDtypeStruct((blocks, width), I32),
            jax.ShapeDtypeStruct((blocks + 1, 16, width), F32),
            jax.ShapeDtypeStruct((room,), I32),
            jax.ShapeDtypeStruct((2 * room,), I32),
            jax.ShapeDtypeStruct((8,), I32),
        ),
        in_specs=[sspec()] * 5 + [vspec()] * 3,
        out_specs=(vspec(),) * 3 + (sspec(),) * 3,
        scratch_shapes=[SMEM((blocks + PAD,), I32), SMEM((2 * (blocks + PAD),), I32), SMEM((blocks + 1,), I32), VMEM((4, width, width), BF16), *buffers()],
        compiler_params=pltpu.CompilerParams(vmem_limit_bytes=60 << 20),
        cost_estimate=pl.CostEstimate(flops=40_000_000, bytes_accessed=4_000_000, transcendentals=12_000_000),
        name="home_pulls",
    )(home_groups, slot, target_groups.T, req, nact, positions, time_bins, tab)

    out = pl.pallas_call(
        remote_kernel,
        out_shape=jax.ShapeDtypeStruct((3, blocks, width), F32),
        in_specs=[sspec()] * 4 + [vspec(), vspec(), hspec(), vspec(), vspec()],
        out_specs=vspec(),
        scratch_shapes=[VMEM((blocks + 1, 16, width), F32), *buffers()],
        compiler_params=pltpu.CompilerParams(vmem_limit_bytes=60 << 20),
        name="remote_pulls",
    )(n, blk, half, nact, fc, reply.reshape(domains * SLOTS, 8, 128), acc, key, positions)
    return jnp.transpose(out, (1, 0, 2))


def solution(mesh):
    return jax.shard_map(
        forces_of,
        mesh=mesh,
        in_specs=(
            P(("dom", "sub"), None, None),
            P(("dom", "sub"), None),
            P(("dom", "sub")),
            P(("dom", "sub"), None),
            P(("dom", "sub"), None),
            P(None, ("dom", "sub")),
            P(("dom", "sub")),
            P("dom", None),
            P("dom"),
        ),
        out_specs=P(("dom", "sub"), None, None),
        check_vma=False,
    )
```

```python
import math

import jax
import jax.numpy as jnp
from jax import lax
from jax.experimental import pallas as pl
from jax.experimental.pallas import tpu as pltpu
from jax.sharding import PartitionSpec as P


CUR_BIN = 2
SOFT = 0.04
F32 = jnp.float32
BF16 = jnp.bfloat16
I32 = jnp.int32

SHIFT = 0.245
POLY = (
    0.999994348,
    -0.564111497,
    0.111462021,
    -0.00487730517,
    -0.00155512244,
    0.000185247258,
)
LEAD = POLY[5]
MONIC = tuple(c / LEAD for c in POLY[:5])
TAIL = 1.0 / (math.sqrt(math.pi) * LEAD)
DECAY = -0.25 * math.log2(math.e)

WIDTHS = (128, 144, 160, 192, 256)
KI = 6
VMEM = pltpu.VMEM
SMEM = pltpu.SMEM
SLOTS = 8


def vspec():
    return pl.BlockSpec(memory_space=VMEM)


def sspec():
    return pl.BlockSpec(memory_space=SMEM)


def hspec():
    return pl.BlockSpec(memory_space=pltpu.MemorySpace.HBM)


def nt_dot(a, b):
    return lax.dot_general(a, b, (((1,), (1,)), ((), ())), preferred_element_type=F32)


def split3(v):
    first = v.astype(BF16).astype(F32)
    rest = v - first
    second = rest.astype(BF16).astype(F32)
    return first, second, rest - second


def fetch(sources, buffers, sems):
    copies = [pltpu.make_async_copy(a, b, sems.at[k]) for k, (a, b) in enumerate(zip(sources, buffers))]
    for copy in copies:
        copy.start()
    return copies


def request_kernel(*refs):
    sources, (req_ref, slot_ref, nact_ref, nodes_ref), held, sems = refs[:6], refs[6:10], refs[10:16], refs[16]
    for copy in fetch(sources, held, sems):
        copy.wait()
    targets_ref, groups_ref, counts_ref, pos_ref, mass_ref, bins_ref = held
    most = targets_ref.shape[0]
    pairs = most * targets_ref.shape[1]
    domains = req_ref.shape[0]

    def in_line(ref):
        return jnp.concatenate([ref[v : v + 1, :] for v in range(most)], axis=1).astype(F32)

    dest = in_line(targets_ref)
    along = jnp.broadcast_to(dest, (pairs, pairs))
    down = jnp.transpose(along)
    earlier = lax.broadcasted_iota(I32, (pairs, pairs), 0) < lax.broadcasted_iota(I32, (pairs, pairs), 1)
    rank = jnp.sum(jnp.where((along == down) & earlier, 1.0, 0.0), axis=0, keepdims=True)
    slot = jnp.where(dest >= 0, dest * SLOTS + rank, -1.0)
    slot_ref[...] = slot.astype(I32)
    active = jnp.where(bins_ref[...] <= CUR_BIN, 1.0, 0.0).astype(BF16)
    nact_ref[...] = nt_dot(jnp.ones((16, active.shape[1]), BF16), active)[0:1].astype(I32)
    dom_id = lax.broadcasted_iota(I32, (domains, pairs), 0).astype(F32)
    asked = in_line(groups_ref) + 1.0
    by_dom = jnp.where(dom_id == dest, asked, 0.0).astype(BF16)
    lane_id = lax.broadcasted_iota(I32, (128, pairs), 0).astype(F32)
    by_rank = jnp.where(lane_id == rank, 1.0, 0.0).astype(BF16)
    wanted = nt_dot(by_dom, by_rank).astype(I32)
    half = counts_ref.shape[1]
    tail = jnp.concatenate([jnp.zeros((1, 128 - half), I32), counts_ref[...]], axis=1)
    lanes = lax.broadcasted_iota(I32, (domains, 128), 1)
    req_ref[...] = jnp.where(lanes < 128 - half, wanted, jnp.broadcast_to(tail, (domains, 128)))
    for r in range(nodes_ref.shape[1]):
        for c in range(3):
            nodes_ref[c, r : r + 1, :] = pos_ref[c : c + 1, 128 * r : 128 * r + 128]
        nodes_ref[3, r : r + 1, :] = mass_ref[0:1, 128 * r : 128 * r + 128]


def list_kernel(*refs):
    chips = len(refs) - 10
    node_refs = refs[:chips]
    lists_hbm, counts_hbm, tab_ref, table_ref, lists_ref, counts_ref, one_ref, *found_refs, sems = refs[chips:]
    _, rows, _ = node_refs[0].shape
    total = chips * rows
    octets = lists_ref.shape[0] // 8
    copies = fetch((lists_hbm, counts_hbm), (lists_ref, counts_ref), sems)
    sharers = lax.axis_size("sub")
    bases = [lax.rem(lax.axis_index("sub") + sharers - 2 * j, sharers) * rows for j in range(chips)]
    for c in range(4):
        tall = jnp.transpose(jnp.concatenate([ref[c] for ref in node_refs], axis=0))
        high = tall.astype(BF16)
        table_ref[128 * c : 128 * c + 128, :total] = high
        table_ref[128 * c : 128 * c + 128, total:] = (tall - high.astype(F32)).astype(BF16)
    for copy in copies:
        copy.wait()
    row16 = lax.broadcasted_iota(I32, (16, 256), 0)
    row8 = lax.broadcasted_iota(I32, (8, 256), 0)
    entry_id = lax.broadcasted_iota(I32, (1, 256), 1)

    def search(one, k):
        at = jnp.broadcast_to(lists_ref[pl.ds(one, 1), :] >> 7, (16, 256))
        for j in range(chips):
            for q in range(0, rows, 16):
                piece = jnp.where(row16 == at - (bases[j] + q), 1.0, 0.0).astype(BF16)
                for part in range(2):
                    put = total * part + rows * j + q
                    one_ref[k % 2, put : put + 16, :] = piece
        found_refs[k % 2][...] = jnp.dot(table_ref[...], one_ref[k % 2], preferred_element_type=F32)

    def select(one, k):
        at = jnp.broadcast_to(lists_ref[pl.ds(one, 1), :] & 127, (8, 256))
        valid = entry_id < counts_ref[one]
        sums = [jnp.zeros((8, 256), F32)] * 4
        for j in range(16):
            here = row8 == at - 8 * j
            for c in range(4):
                piece = found_refs[k % 2][128 * c + 8 * j : 128 * c + 8 * j + 8, :]
                sums[c] = sums[c] + jnp.where(here, piece, 0.0)
        for c in range(4):
            value = jnp.where(valid, jnp.sum(sums[c], axis=0, keepdims=True), 0.0)
            for h in range(2):
                tab_ref[one, 4 * h + c : 4 * h + c + 1, :] = value[:, 128 * h : 128 * h + 128]

    found_refs[1][...] = jnp.zeros(found_refs[1].shape, F32)

    def gather(i, carry):
        first = i * 8
        for k in range(8):
            search(first + k, k)
            select(jnp.maximum(first + k - 1, 0), k + 1)
        return carry

    lax.fori_loop(0, octets, gather, 0)
    select(8 * octets - 1, 1)


def build_lists(nodes, node_lists, list_counts):
    lists = node_lists.shape[0]
    deep = 2 * len(nodes) * nodes[0].shape[1]
    return pl.pallas_call(
        list_kernel,
        out_shape=jax.ShapeDtypeStruct((lists, 8, 128), F32),
        in_specs=[vspec()] * len(nodes) + [hspec(), hspec()],
        out_specs=vspec(),
        scratch_shapes=[
            VMEM((512, deep), BF16),
            VMEM(node_lists.shape, I32),
            SMEM(list_counts.shape, I32),
            VMEM((2, deep, 256), BF16),
            VMEM((512, 256), F32),
            VMEM((512, 256), F32),
            pltpu.SemaphoreType.DMA((2,)),
        ],
        compiler_params=pltpu.CompilerParams(vmem_limit_bytes=60 << 20),
        cost_estimate=pl.CostEstimate(flops=20_000_000, bytes_accessed=1_000_000, transcendentals=0),
        name="lists",
    )(*nodes, node_lists, list_counts)


def pack_kernel(req_ref, mine_ref, theirs_ref, tab_ref, reply_ref):
    tab_ref[...] = mine_ref[...] + theirs_ref[...]

    def pack(d, carry):
        for u in range(4):
            for j in range(SLOTS):
                group = jnp.maximum(req_ref[4 * d + u, j] - 1, 0)
                reply_ref[4 * d + u, j] = tab_ref[group]
        return carry

    lax.fori_loop(0, reply_ref.shape[0] // 4, pack, 0)


def row_masks():
    row = lax.broadcasted_iota(I32, (8, 128), 0)
    return row < 4, row % 4 == 3, row


def list_features(tile):
    low, last, row = row_masks()
    sq = tile * tile
    norm = pltpu.roll(sq, 1, 0) + pltpu.roll(sq, 2, 0) + pltpu.roll(sq, 3, 0)
    g = split3(jnp.where(last, norm, tile))
    ga = [pltpu.roll(v, 4, 0) for v in g]

    def pair(a, b, h):
        if h == 0:
            return jnp.where(low, g[a], ga[b])
        return jnp.where(low, ga[a], g[b])

    ones = jnp.where(row < 3, 1.0, 0.0)
    feats = jnp.concatenate(
        [
            jnp.concatenate([pair(0, 0, h), pair(0, 1, h), pair(1, 2, h), ones], axis=0)
            for h in range(2)
        ],
        axis=1,
    ).astype(BF16)
    m1, m2, m3 = pltpu.roll(tile, 7, 0), pltpu.roll(tile, 6, 0), pltpu.roll(tile, 5, 0)
    col = row % 4
    mass = jnp.where(col == 0, m3, jnp.where(col == 1, m2, m1))
    w = split3(jnp.where(last, tile, tile * mass))
    wa = [pltpu.roll(v, 4, 0) for v in w]
    zero = jnp.zeros((8, 128), F32)
    loaded = jnp.concatenate(
        [
            jnp.concatenate(
                [
                    jnp.where(low, w[0], wa[1]) if h == 0 else jnp.where(low, wa[0], w[1]),
                    jnp.where(low, w[2] if h == 0 else wa[2], zero),
                ],
                axis=0,
            )
            for h in range(2)
        ],
        axis=1,
    ).astype(BF16)
    return feats, loaded


def weights(s):
    q = lax.rsqrt(s)
    t = 1.0 / (q + SHIFT)
    p = t + MONIC[4]
    for k in (3, 2, 1, 0):
        p = p * t + MONIC[k]
    e = jnp.exp2(s * DECAY)
    return (q * q) * e * (q * p + TAIL)


def run_items(groups, blk_ref, half_ref, nact_ref, fc_ref, tab_ref, acc_ref, bufs, ready=None):
    last_block = fc_ref.shape[0] - 1
    nobody = acc_ref.shape[0] - 1
    s_bufs, y_bufs, w_buf = bufs
    last = KI - 1

    def active_in(i):
        return nact_ref[jnp.minimum(blk_ref[i], last_block)]

    def two_halves(first, second):
        low, _, _ = row_masks()
        a = tab_ref[first >> 1]
        b = tab_ref[jnp.maximum(second, 0) >> 1]
        a = jnp.where((first & 1) == 1, pltpu.roll(a, 4, 0), a)
        b = jnp.where((second & 1) == 1, b, pltpu.roll(b, 4, 0))
        return jnp.where(low, a, jnp.where(second >= 0, b, 0.0))

    def prepare(g, k, par, width):
        i = g * KI + k
        b = jnp.minimum(blk_ref[i], last_block)
        feats, loaded = list_features(two_halves(half_ref[2 * i], half_ref[2 * i + 1]))
        y_bufs[par][k][...] = loaded
        wide = 128 if width == 128 else 256
        columns = jnp.transpose(fc_ref[b, :, :wide])[:width]
        s_bufs[par][k][:width, :] = jnp.dot(columns, feats, preferred_element_type=F32)

    def split_weights(k, par, width):
        for j in range(0, width, 16):
            w = weights(s_bufs[par][k][j : j + 16, :])
            hi = w.astype(BF16)
            yield j, hi, (w - hi.astype(F32)).astype(BF16)

    def reduce(k, par, width):
        pieces = list(split_weights(k, par, width))
        loaded = y_bufs[par][k][...]
        hi = jnp.concatenate([p[1] for p in pieces], axis=0)
        lo = jnp.concatenate([p[2] for p in pieces], axis=0)
        return nt_dot(loaded, hi) + nt_dot(loaded, lo)

    def leave(par, width):
        for j, hi, lo in split_weights(last, par, width):
            w_buf[0, j : j + 16, :] = hi
            w_buf[1, j : j + 16, :] = lo

    def left(par, width):
        loaded = y_bufs[par][last][...]
        return nt_dot(loaded, w_buf[0, :width, :]) + nt_dot(loaded, w_buf[1, :width, :])

    def add(b, made, width):
        acc_ref[b, :, :width] = acc_ref[b, :, :width] + made

    def before(g):
        return jnp.where(g > 0, blk_ref[jnp.maximum(g * KI - 1, 0)], nobody)

    def by_width(n, body):
        low = -1
        for width in WIDTHS:
            @pl.when((n > low) & (n <= width))
            def _(width=width):
                body(width)

            low = width

    def step(g, par):
        n = nact_ref[jnp.minimum(before(g), last_block)]
        for k in range(2 * KI):
            n = jnp.maximum(n, active_in(g * KI + k))

        def body(width):
            old = left(1 - par, width)
            made = []
            for k in range(KI):
                prepare(g + 1, k, 1 - par, width)
            for k in range(KI):
                if k < last:
                    made.append(reduce(k, par, width))
                else:
                    leave(par, width)
            add(before(g), old, width)
            for k in range(last):
                add(blk_ref[g * KI + k], made[k], width)

        by_width(n, body)

    def two_steps(gg, carry):
        step(2 * gg, 0)
        step(2 * gg + 1, 1)
        return carry

    w_buf[...] = jnp.zeros(w_buf.shape, BF16)
    y_bufs[1][last][...] = jnp.zeros(y_bufs[1][last].shape, BF16)
    for k in range(KI):
        prepare(0, k, 0, 256)
    if ready is not None:
        ready()
    lax.fori_loop(0, (groups + 1) // 2, two_steps, 0)
    add(before(2 * ((groups + 1) // 2)), left(1, 256), 256)


def buffers():
    return (
        *[VMEM((256, 256), F32) for _ in range(2 * KI)],
        *[VMEM((16, 256), BF16) for _ in range(2 * KI)],
        VMEM((2, 256, 256), BF16),
    )


def take_buffers(flat):
    s, y = flat[: 2 * KI], flat[2 * KI : -1]
    return (s[:KI], s[KI:]), (y[:KI], y[KI:]), flat[-1]


PAD = 4 * KI


def home_kernel(
    home_ref, slot_ref, groups_ref, req_ref, nact_ref, pos_ref, bins_ref, tab_ref,
    fc_ref, key_ref, acc_ref, blk_out, half_out, n_out, blk_ref, half_ref, order_ref, chosen_ref, *flat
):
    _, blocks, width = pos_ref.shape
    active = bins_ref[...] <= CUR_BIN
    tri = lax.broadcasted_iota(I32, (width, width), 0) <= lax.broadcasted_iota(I32, (width, width), 1)
    upto = jnp.dot(
        jnp.where(active, 1.0, 0.0).astype(BF16),
        jnp.where(tri, 1.0, 0.0).astype(BF16),
        preferred_element_type=F32,
    )
    key_ref[...] = jnp.where(active, upto - 1.0, -1.0).astype(I32)

    low8 = lax.broadcasted_iota(I32, (8, width), 0) < 4
    row8 = lax.broadcasted_iota(I32, (8, width), 0)
    row16 = lax.broadcasted_iota(I32, (16, width), 0)

    def compact(bb, carry):
        for u in range(4):
            b = bb * 4 + u
            key = jnp.broadcast_to(key_ref[pl.ds(b, 1), :], (16, width))
            for j in range(0, width, 16):
                chosen_ref[u, j : j + 16, :] = jnp.where(row16 == key - j, 1.0, 0.0).astype(BF16)
            pos = jnp.concatenate(
                [pos_ref[c, pl.ds(b, 1), :] for c in range(3)] + [jnp.zeros((5, width), F32)], axis=0
            )
            parts = jnp.concatenate(split3(pos), axis=0).astype(BF16)
            moved = nt_dot(parts, chosen_ref[u])
            x = (moved[0:8] + moved[8:16]) + moved[16:24]
            sq = x * x
            norm = sq[0:1] + sq[1:2] + sq[2:3] + SOFT
            n1, n2, n3 = split3(norm)
            a1, a2, a3 = split3(x * -2.0)
            unit = jnp.where(row8 == 3, 1.0, 0.0)
            a1 = a1 + unit
            r1, r2 = pltpu.roll(a1, 4, 0), pltpu.roll(a2, 4, 0)
            feats = jnp.concatenate(
                [
                    jnp.where(low8, a1, r2),
                    jnp.where(low8, a3, r1),
                    jnp.where(low8, a2, r1),
                    jnp.concatenate([n1, n2, n3, jnp.zeros((5, width), F32)], axis=0),
                ],
                axis=0,
            )
            fc_ref[b] = feats.astype(BF16)
            acc_ref[b] = jnp.zeros((16, width), F32)
        return carry

    lax.fori_loop(0, blocks // 4, compact, 0)
    acc_ref[blocks] = jnp.zeros((16, width), F32)

    def home_item(i, carry):
        inside = i < blocks
        b = jnp.minimum(i, blocks - 1)
        blk_ref[i] = jnp.where(inside, i, blocks)
        half_ref[2 * i] = 2 * home_ref[b]
        half_ref[2 * i + 1] = 2 * home_ref[b] + 1
        return carry

    lax.fori_loop(0, blocks + PAD, home_item, 0)
    run_items((blocks + KI - 1) // KI, blk_ref, half_ref, nact_ref, fc_ref, tab_ref, acc_ref, take_buffers(flat))

    most = slot_ref.shape[1] // blocks
    lists = 128 // 2

    where = I32(0)
    low = -1
    for high in (WIDTHS[0], WIDTHS[1], WIDTHS[-1]):

        def place_block(b, n, low=low, high=high):
            order_ref[n] = b
            return n + jnp.where((nact_ref[b] > low) & (nact_ref[b] <= high), 1, 0)

        where = lax.fori_loop(0, blocks, place_block, where)
        low = high

    def visits(at, n):
        b = order_ref[at]
        for v in range(most):
            slot = slot_ref[0, v * blocks + b]
            used = jnp.where(slot >= 0, 1, 0)
            place = jnp.maximum(slot, 0)
            count = req_ref[place >> 3, lists + groups_ref[v, b]]
            blk_out[n >> 1] = b
            half_out[n] = 2 * place
            n = n + used
            blk_out[n >> 1] = b
            half_out[n] = 2 * place + 1
            n = n + jnp.where(count > 128, used, 0)
        half_out[n] = -1
        return n + (n & 1)

    end = lax.fori_loop(0, blocks, visits, I32(0)) >> 1

    def no_item(k, carry):
        blk_out[k] = blocks
        half_out[2 * k] = 0
        half_out[2 * k + 1] = -1
        return carry

    lax.fori_loop(end, end + PAD, no_item, 0)
    n_out[0] = end


def remote_kernel(n_ref, blk_ref, half_ref, nact_ref, fc_ref, tab_ref, acc_in_ref, key_ref, pos_ref, out_ref, acc_ref, sem, *flat):
    blocks = pos_ref.shape[1]
    copy = pltpu.make_async_copy(acc_in_ref, acc_ref, sem)
    copy.start()
    run_items(
        (n_ref[0] + KI - 1) // KI,
        blk_ref,
        half_ref,
        nact_ref,
        fc_ref,
        tab_ref,
        acc_ref,
        take_buffers(flat),
        copy.wait,
    )

    def finish(bb, carry):
        for u in range(4):
            b = bb * 4 + u
            acc = acc_ref[b]
            top = acc[0:8]
            total = top + pltpu.roll(top, 4, 0) + acc[8:16]
            key = key_ref[pl.ds(b, 1), :]
            parts = []
            for h in range(2):
                at = jnp.broadcast_to(key[:, 128 * h : 128 * h + 128], (8, 128))
                lane = at & 127
                left = jnp.take_along_axis(total[:, :128], lane, axis=1, mode="promise_in_bounds")
                right = jnp.take_along_axis(total[:, 128:], lane, axis=1, mode="promise_in_bounds")
                parts.append(jnp.where(at < 128, left, right))
            back = jnp.concatenate(parts, axis=1)
            for c in range(3):
                pull = (back[c : c + 1] - pos_ref[c, pl.ds(b, 1), :] * back[3:4]) * LEAD
                out_ref[c, pl.ds(b, 1), :] = jnp.where(key >= 0, pull, 0.0)
        return carry

    lax.fori_loop(0, blocks // 4, finish, 0)


def forces_of(positions, time_bins, home_groups, targets, target_groups, node_pos, node_mass, node_lists, list_counts):
    domains = lax.axis_size("dom")
    sharers = lax.axis_size("sub")
    blocks, most = targets.shape
    pairs = blocks * most
    width = positions.shape[2]
    lists = node_lists.shape[0]
    rows = node_mass.shape[0] // 128

    asked = (targets.T, target_groups.T, list_counts.reshape(1, lists), node_pos, node_mass.reshape(1, -1), time_bins)
    req, slot, nact, nodes = pl.pallas_call(
        request_kernel,
        out_shape=(
            jax.ShapeDtypeStruct((domains, 128), I32),
            jax.ShapeDtypeStruct((1, pairs), I32),
            jax.ShapeDtypeStruct((1, blocks), I32),
            jax.ShapeDtypeStruct((4, rows, 128), F32),
        ),
        in_specs=[hspec()] * 6,
        out_specs=(vspec(),) * 4,
        scratch_shapes=[*[VMEM(a.shape, a.dtype) for a in asked], pltpu.SemaphoreType.DMA((6,))],
        compiler_params=pltpu.CompilerParams(vmem_limit_bytes=60 << 20),
        name="requests",
    )(*asked)
    held = [nodes]
    for j in range(1, sharers // 2):
        held.append(lax.ppermute(nodes, "sub", [(i, (i + 2 * j) % sharers) for i in range(sharers)]))
    req = lax.all_to_all(req.reshape(domains, 1, 128), "dom", 0, 0, tiled=True)
    req = req.reshape(domains, 128)
    nact = nact.reshape(blocks)

    mine = build_lists(held, node_lists, list_counts)
    theirs = lax.ppermute(mine, "sub", [(i, i ^ 1) for i in range(sharers)])
    tab, reply = pl.pallas_call(
        pack_kernel,
        out_shape=(
            jax.ShapeDtypeStruct((lists, 8, 128), F32),
            jax.ShapeDtypeStruct((domains, SLOTS, 8, 128), F32),
        ),
        in_specs=[sspec(), vspec(), vspec()],
        out_specs=(vspec(),) * 2,
        compiler_params=pltpu.CompilerParams(vmem_limit_bytes=60 << 20),
        name="pack",
    )(req, mine, theirs)
    reply = lax.all_to_all(reply.reshape(domains, SLOTS * 8, 128), "dom", 0, 0, tiled=True)

    positions = jnp.transpose(positions, (1, 0, 2))
    room = pairs + PAD
    fc, key, acc, blk, half, n = pl.pallas_call(
        home_kernel,
        out_shape=(
            jax.ShapeDtypeStruct((blocks, 32, width), BF16),
            jax.ShapeDtypeStruct((blocks, width), I32),
            jax.ShapeDtypeStruct((blocks + 1, 16, width), F32),
            jax.ShapeDtypeStruct((room,), I32),
            jax.ShapeDtypeStruct((2 * room,), I32),
            jax.ShapeDtypeStruct((8,), I32),
        ),
        in_specs=[sspec()] * 5 + [vspec()] * 3,
        out_specs=(vspec(),) * 3 + (sspec(),) * 3,
        scratch_shapes=[SMEM((blocks + PAD,), I32), SMEM((2 * (blocks + PAD),), I32), SMEM((blocks + 1,), I32), VMEM((4, width, width), BF16), *buffers()],
        compiler_params=pltpu.CompilerParams(vmem_limit_bytes=65136 << 10),
        cost_estimate=pl.CostEstimate(flops=40_000_000, bytes_accessed=4_000_000, transcendentals=12_000_000),
        name="home_pulls",
    )(home_groups, slot, target_groups.T, req, nact, positions, time_bins, tab)

    out = pl.pallas_call(
        remote_kernel,
        out_shape=jax.ShapeDtypeStruct((3, blocks, width), F32),
        in_specs=[sspec()] * 4 + [vspec(), vspec(), hspec(), vspec(), vspec()],
        out_specs=vspec(),
        scratch_shapes=[VMEM((blocks + 1, 16, width), F32), pltpu.SemaphoreType.DMA, *buffers()],
        compiler_params=pltpu.CompilerParams(vmem_limit_bytes=60 << 20),
        name="remote_pulls",
    )(n, blk, half, nact, fc, reply.reshape(domains * SLOTS, 8, 128), acc, key, positions)
    return jnp.transpose(out, (1, 0, 2))


def solution(mesh):
    return jax.shard_map(
        forces_of,
        mesh=mesh,
        in_specs=(
            P(("dom", "sub"), None, None),
            P(("dom", "sub"), None),
            P(("dom", "sub")),
            P(("dom", "sub"), None),
            P(("dom", "sub"), None),
            P(None, ("dom", "sub")),
            P(("dom", "sub")),
            P("dom", None),
            P("dom"),
        ),
        out_specs=P(("dom", "sub"), None, None),
        check_vma=False,
    )
```

```python
import math

import jax
import jax.numpy as jnp
from jax import lax
from jax.experimental import pallas as pl
from jax.experimental.pallas import tpu as pltpu
from jax.sharding import PartitionSpec as P


CUR_BIN = 2
SOFT = 0.04
F32 = jnp.float32
BF16 = jnp.bfloat16
I32 = jnp.int32

SHIFT = 0.245
POLY = (
    0.999994348,
    -0.564111497,
    0.111462021,
    -0.00487730517,
    -0.00155512244,
    0.000185247258,
)
LEAD = POLY[5]
MONIC = tuple(c / LEAD for c in POLY[:5])
TAIL = 1.0 / (math.sqrt(math.pi) * LEAD)
DECAY = -0.25 * math.log2(math.e)

WIDTHS = (128, 144, 160, 256)
KI = 8
VMEM = pltpu.VMEM
SMEM = pltpu.SMEM
SLOTS = 8


def vspec():
    return pl.BlockSpec(memory_space=VMEM)


def sspec():
    return pl.BlockSpec(memory_space=SMEM)


def hspec():
    return pl.BlockSpec(memory_space=pltpu.MemorySpace.HBM)


def nt_dot(a, b):
    return lax.dot_general(a, b, (((1,), (1,)), ((), ())), preferred_element_type=F32)


def split3(v):
    first = v.astype(BF16).astype(F32)
    rest = v - first
    second = rest.astype(BF16).astype(F32)
    return first, second, rest - second


def fetch(sources, buffers, sems):
    copies = [pltpu.make_async_copy(a, b, sems.at[k]) for k, (a, b) in enumerate(zip(sources, buffers))]
    for copy in copies:
        copy.start()
    return copies


def request_kernel(*refs):
    sources, (req_ref, slot_ref, nact_ref, nodes_ref), held, sems = refs[:6], refs[6:10], refs[10:16], refs[16]
    for copy in fetch(sources, held, sems):
        copy.wait()
    targets_ref, groups_ref, counts_ref, pos_ref, mass_ref, bins_ref = held
    most = targets_ref.shape[0]
    pairs = most * targets_ref.shape[1]
    domains = req_ref.shape[0]

    def in_line(ref):
        return jnp.concatenate([ref[v : v + 1, :] for v in range(most)], axis=1).astype(F32)

    dest = in_line(targets_ref)
    along = jnp.broadcast_to(dest, (pairs, pairs))
    down = jnp.transpose(along)
    earlier = lax.broadcasted_iota(I32, (pairs, pairs), 0) < lax.broadcasted_iota(I32, (pairs, pairs), 1)
    rank = jnp.sum(jnp.where((along == down) & earlier, 1.0, 0.0), axis=0, keepdims=True)
    slot = jnp.where(dest >= 0, dest * SLOTS + rank, -1.0)
    slot_ref[...] = slot.astype(I32)
    active = jnp.where(bins_ref[...] <= CUR_BIN, 1.0, 0.0).astype(BF16)
    nact_ref[...] = nt_dot(jnp.ones((16, active.shape[1]), BF16), active)[0:1].astype(I32)
    dom_id = lax.broadcasted_iota(I32, (domains, pairs), 0).astype(F32)
    asked = in_line(groups_ref) + 1.0
    by_dom = jnp.where(dom_id == dest, asked, 0.0).astype(BF16)
    lane_id = lax.broadcasted_iota(I32, (128, pairs), 0).astype(F32)
    by_rank = jnp.where(lane_id == rank, 1.0, 0.0).astype(BF16)
    wanted = nt_dot(by_dom, by_rank).astype(I32)
    half = counts_ref.shape[1]
    tail = jnp.concatenate([jnp.zeros((1, 128 - half), I32), counts_ref[...]], axis=1)
    lanes = lax.broadcasted_iota(I32, (domains, 128), 1)
    req_ref[...] = jnp.where(lanes < 128 - half, wanted, jnp.broadcast_to(tail, (domains, 128)))
    for r in range(nodes_ref.shape[1]):
        for c in range(3):
            nodes_ref[c, r : r + 1, :] = pos_ref[c : c + 1, 128 * r : 128 * r + 128]
        nodes_ref[3, r : r + 1, :] = mass_ref[0:1, 128 * r : 128 * r + 128]


def list_kernel(*refs):
    chips = len(refs) - 10
    node_refs = refs[:chips]
    lists_hbm, counts_hbm, tab_ref, table_ref, lists_ref, counts_ref, one_ref, *found_refs, sems = refs[chips:]
    _, rows, _ = node_refs[0].shape
    total = chips * rows
    octets = lists_ref.shape[0] // 8
    copies = fetch((lists_hbm, counts_hbm), (lists_ref, counts_ref), sems)
    sharers = lax.axis_size("sub")
    bases = [lax.rem(lax.axis_index("sub") + sharers - 2 * j, sharers) * rows for j in range(chips)]
    for c in range(4):
        tall = jnp.transpose(jnp.concatenate([ref[c] for ref in node_refs], axis=0))
        high = tall.astype(BF16)
        table_ref[128 * c : 128 * c + 128, :total] = high
        table_ref[128 * c : 128 * c + 128, total:] = (tall - high.astype(F32)).astype(BF16)
    for copy in copies:
        copy.wait()
    row16 = lax.broadcasted_iota(I32, (16, 256), 0)
    row8 = lax.broadcasted_iota(I32, (8, 256), 0)
    entry_id = lax.broadcasted_iota(I32, (1, 256), 1)

    def search(one, k):
        at = jnp.broadcast_to(lists_ref[pl.ds(one, 1), :] >> 7, (16, 256))
        for j in range(chips):
            for q in range(0, rows, 16):
                piece = jnp.where(row16 == at - (bases[j] + q), 1.0, 0.0).astype(BF16)
                for part in range(2):
                    put = total * part + rows * j + q
                    one_ref[k % 2, put : put + 16, :] = piece
        found_refs[k % 2][...] = jnp.dot(table_ref[...], one_ref[k % 2], preferred_element_type=F32)

    def select(one, k):
        at = jnp.broadcast_to(lists_ref[pl.ds(one, 1), :] & 127, (8, 256))
        valid = entry_id < counts_ref[one]
        sums = [jnp.zeros((8, 256), F32)] * 4
        for j in range(16):
            here = row8 == at - 8 * j
            for c in range(4):
                piece = found_refs[k % 2][128 * c + 8 * j : 128 * c + 8 * j + 8, :]
                sums[c] = sums[c] + jnp.where(here, piece, 0.0)
        for c in range(4):
            value = jnp.where(valid, jnp.sum(sums[c], axis=0, keepdims=True), 0.0)
            for h in range(2):
                tab_ref[one, 4 * h + c : 4 * h + c + 1, :] = value[:, 128 * h : 128 * h + 128]

    found_refs[1][...] = jnp.zeros(found_refs[1].shape, F32)

    def gather(i, carry):
        first = i * 8
        for k in range(8):
            search(first + k, k)
            select(jnp.maximum(first + k - 1, 0), k + 1)
        return carry

    lax.fori_loop(0, octets, gather, 0)
    select(8 * octets - 1, 1)


def build_lists(nodes, node_lists, list_counts):
    lists = node_lists.shape[0]
    deep = 2 * len(nodes) * nodes[0].shape[1]
    return pl.pallas_call(
        list_kernel,
        out_shape=jax.ShapeDtypeStruct((lists, 8, 128), F32),
        in_specs=[vspec()] * len(nodes) + [hspec(), hspec()],
        out_specs=vspec(),
        scratch_shapes=[
            VMEM((512, deep), BF16),
            VMEM(node_lists.shape, I32),
            SMEM(list_counts.shape, I32),
            VMEM((2, deep, 256), BF16),
            VMEM((512, 256), F32),
            VMEM((512, 256), F32),
            pltpu.SemaphoreType.DMA((2,)),
        ],
        compiler_params=pltpu.CompilerParams(vmem_limit_bytes=60 << 20),
        cost_estimate=pl.CostEstimate(flops=20_000_000, bytes_accessed=1_000_000, transcendentals=0),
        name="lists",
    )(*nodes, node_lists, list_counts)


def pack_kernel(req_ref, mine_ref, theirs_ref, reply_hbm, reply_ref, sems):
    each = reply_ref.shape[0] // sems.shape[0]

    def chunk(d):
        return pltpu.make_async_copy(
            reply_ref.at[pl.ds(each * d, each)], reply_hbm.at[pl.ds(each * d, each)], sems.at[d]
        )

    for d in range(sems.shape[0]):
        for u in range(each):
            for j in range(SLOTS):
                group = jnp.maximum(req_ref[each * d + u, j] - 1, 0)
                reply_ref[each * d + u, j] = mine_ref[group] + theirs_ref[group]
        chunk(d).start()
    for d in range(sems.shape[0]):
        chunk(d).wait()


def row_masks():
    row = lax.broadcasted_iota(I32, (8, 128), 0)
    return row < 4, row % 4 == 3, row


def list_features(tile):
    low, last, row = row_masks()
    sq = tile * tile
    norm = pltpu.roll(sq, 1, 0) + pltpu.roll(sq, 2, 0) + pltpu.roll(sq, 3, 0)
    g = split3(jnp.where(last, norm, tile))
    ga = [pltpu.roll(v, 4, 0) for v in g]

    def pair(a, b, h):
        if h == 0:
            return jnp.where(low, g[a], ga[b])
        return jnp.where(low, ga[a], g[b])

    ones = jnp.where(row < 3, 1.0, 0.0)
    feats = jnp.concatenate(
        [
            jnp.concatenate([pair(0, 0, h), pair(0, 1, h), pair(1, 2, h), ones], axis=0)
            for h in range(2)
        ],
        axis=1,
    ).astype(BF16)
    m1, m2, m3 = pltpu.roll(tile, 7, 0), pltpu.roll(tile, 6, 0), pltpu.roll(tile, 5, 0)
    col = row % 4
    mass = jnp.where(col == 0, m3, jnp.where(col == 1, m2, m1))
    w = split3(jnp.where(last, tile, tile * mass))
    wa = [pltpu.roll(v, 4, 0) for v in w]
    zero = jnp.zeros((8, 128), F32)
    loaded = jnp.concatenate(
        [
            jnp.concatenate(
                [
                    jnp.where(low, w[0], wa[1]) if h == 0 else jnp.where(low, wa[0], w[1]),
                    jnp.where(low, w[2] if h == 0 else wa[2], zero),
                ],
                axis=0,
            )
            for h in range(2)
        ],
        axis=1,
    ).astype(BF16)
    return feats, loaded


def weights(s):
    q = lax.rsqrt(s)
    t = 1.0 / (q + SHIFT)
    p = t + MONIC[4]
    for k in (3, 2, 1, 0):
        p = p * t + MONIC[k]
    e = jnp.exp2(s * DECAY)
    return (q * q) * e * (q * p + TAIL)


def run_items(groups, blk_ref, half_ref, nact_ref, fc_ref, list_tile, acc_ref, bufs, ready=None):
    last_block = fc_ref.shape[0] - 1
    nobody = acc_ref.shape[0] - 1
    s_bufs, y_bufs, w_buf = bufs
    last = KI - 1

    def active_in(i):
        return nact_ref[jnp.minimum(blk_ref[i], last_block)]

    def two_halves(first, second):
        low, _, _ = row_masks()
        a = list_tile(first >> 1)
        b = list_tile(jnp.maximum(second, 0) >> 1)
        a = jnp.where((first & 1) == 1, pltpu.roll(a, 4, 0), a)
        b = jnp.where((second & 1) == 1, b, pltpu.roll(b, 4, 0))
        return jnp.where(low, a, jnp.where(second >= 0, b, 0.0))

    def prepare(g, k, par, width):
        i = g * KI + k
        b = jnp.minimum(blk_ref[i], last_block)
        feats, loaded = list_features(two_halves(half_ref[2 * i], half_ref[2 * i + 1]))
        y_bufs[par][k][...] = loaded
        wide = 128 if width == 128 else 256
        columns = jnp.transpose(fc_ref[b, :, :wide])[:width]
        s_bufs[par][k][:width, :] = jnp.dot(columns, feats, preferred_element_type=F32)

    def split_weights(k, par, width):
        for j in range(0, width, 16):
            w = weights(s_bufs[par][k][j : j + 16, :])
            hi = w.astype(BF16)
            yield j, hi, (w - hi.astype(F32)).astype(BF16)

    def reduce(k, par, width):
        pieces = list(split_weights(k, par, width))
        loaded = y_bufs[par][k][...]
        hi = jnp.concatenate([p[1] for p in pieces], axis=0)
        lo = jnp.concatenate([p[2] for p in pieces], axis=0)
        return nt_dot(loaded, hi) + nt_dot(loaded, lo)

    def leave(par, width):
        for j, hi, lo in split_weights(last, par, width):
            w_buf[0, j : j + 16, :] = hi
            w_buf[1, j : j + 16, :] = lo

    def left(par, width):
        loaded = y_bufs[par][last][...]
        return nt_dot(loaded, w_buf[0, :width, :]) + nt_dot(loaded, w_buf[1, :width, :])

    def add(b, made, width):
        acc_ref[b, :, :width] = acc_ref[b, :, :width] + made

    def before(g):
        return jnp.where(g > 0, blk_ref[jnp.maximum(g * KI - 1, 0)], nobody)

    def by_width(n, body):
        low = -1
        for width in WIDTHS:
            @pl.when((n > low) & (n <= width))
            def _(width=width):
                body(width)

            low = width

    def step(g, par):
        n = nact_ref[jnp.minimum(before(g), last_block)]
        for k in range(2 * KI):
            n = jnp.maximum(n, active_in(g * KI + k))

        def body(width):
            old = left(1 - par, width)
            made = []
            for k in range(KI):
                prepare(g + 1, k, 1 - par, width)
            for k in range(KI):
                if k < last:
                    made.append(reduce(k, par, width))
                else:
                    leave(par, width)
            add(before(g), old, width)
            for k in range(last):
                add(blk_ref[g * KI + k], made[k], width)

        by_width(n, body)

    def two_steps(gg, carry):
        step(2 * gg, 0)
        step(2 * gg + 1, 1)
        return carry

    w_buf[...] = jnp.zeros(w_buf.shape, BF16)
    y_bufs[1][last][...] = jnp.zeros(y_bufs[1][last].shape, BF16)
    for k in range(KI):
        prepare(0, k, 0, 256)
    if ready is not None:
        ready()
    lax.fori_loop(0, (groups + 1) // 2, two_steps, 0)
    add(before(2 * ((groups + 1) // 2)), left(1, 256), 256)


def buffers():
    return (
        *[VMEM((256, 256), F32) for _ in range(2 * KI)],
        *[VMEM((16, 256), BF16) for _ in range(2 * KI)],
        VMEM((2, 256, 256), BF16),
    )


def take_buffers(flat):
    s, y = flat[: 2 * KI], flat[2 * KI : -1]
    return (s[:KI], s[KI:]), (y[:KI], y[KI:]), flat[-1]


PAD = 4 * KI


def home_kernel(
    home_ref, slot_ref, groups_ref, req_ref, nact_ref, pos_ref, bins_ref, mine_ref, theirs_ref,
    fc_ref, key_ref, acc_ref, blk_out, half_out, n_out, blk_ref, half_ref, order_ref, chosen_ref, *flat
):
    _, blocks, width = pos_ref.shape
    active = bins_ref[...] <= CUR_BIN
    tri = lax.broadcasted_iota(I32, (width, width), 0) <= lax.broadcasted_iota(I32, (width, width), 1)
    upto = jnp.dot(
        jnp.where(active, 1.0, 0.0).astype(BF16),
        jnp.where(tri, 1.0, 0.0).astype(BF16),
        preferred_element_type=F32,
    )
    key_ref[...] = jnp.where(active, upto - 1.0, -1.0).astype(I32)

    low8 = lax.broadcasted_iota(I32, (8, width), 0) < 4
    row8 = lax.broadcasted_iota(I32, (8, width), 0)
    row16 = lax.broadcasted_iota(I32, (16, width), 0)

    def compact(bb, carry):
        for u in range(4):
            b = bb * 4 + u
            key = jnp.broadcast_to(key_ref[pl.ds(b, 1), :], (16, width))
            for j in range(0, width, 16):
                chosen_ref[u, j : j + 16, :] = jnp.where(row16 == key - j, 1.0, 0.0).astype(BF16)
            pos = jnp.concatenate(
                [pos_ref[c, pl.ds(b, 1), :] for c in range(3)] + [jnp.zeros((5, width), F32)], axis=0
            )
            parts = jnp.concatenate(split3(pos), axis=0).astype(BF16)
            moved = nt_dot(parts, chosen_ref[u])
            x = (moved[0:8] + moved[8:16]) + moved[16:24]
            sq = x * x
            norm = sq[0:1] + sq[1:2] + sq[2:3] + SOFT
            n1, n2, n3 = split3(norm)
            a1, a2, a3 = split3(x * -2.0)
            unit = jnp.where(row8 == 3, 1.0, 0.0)
            a1 = a1 + unit
            r1, r2 = pltpu.roll(a1, 4, 0), pltpu.roll(a2, 4, 0)
            feats = jnp.concatenate(
                [
                    jnp.where(low8, a1, r2),
                    jnp.where(low8, a3, r1),
                    jnp.where(low8, a2, r1),
                    jnp.concatenate([n1, n2, n3, jnp.zeros((5, width), F32)], axis=0),
                ],
                axis=0,
            )
            fc_ref[b] = feats.astype(BF16)
            acc_ref[b] = jnp.zeros((16, width), F32)
        return carry

    lax.fori_loop(0, blocks // 4, compact, 0)
    acc_ref[blocks] = jnp.zeros((16, width), F32)

    def home_item(i, carry):
        inside = i < blocks
        b = jnp.minimum(i, blocks - 1)
        blk_ref[i] = jnp.where(inside, i, blocks)
        half_ref[2 * i] = 2 * home_ref[b]
        half_ref[2 * i + 1] = 2 * home_ref[b] + 1
        return carry

    lax.fori_loop(0, blocks + PAD, home_item, 0)
    run_items(
        (blocks + KI - 1) // KI,
        blk_ref,
        half_ref,
        nact_ref,
        fc_ref,
        lambda one: mine_ref[one] + theirs_ref[one],
        acc_ref,
        take_buffers(flat),
    )

    most = slot_ref.shape[1] // blocks
    lists = 128 // 2

    where = I32(0)
    low = -1
    for high in (WIDTHS[0], WIDTHS[1], WIDTHS[-1]):

        def place_block(b, n, low=low, high=high):
            order_ref[n] = b
            return n + jnp.where((nact_ref[b] > low) & (nact_ref[b] <= high), 1, 0)

        where = lax.fori_loop(0, blocks, place_block, where)
        low = high

    def visits(at, n):
        b = order_ref[at]
        for v in range(most):
            slot = slot_ref[0, v * blocks + b]
            used = jnp.where(slot >= 0, 1, 0)
            place = jnp.maximum(slot, 0)
            count = req_ref[place >> 3, lists + groups_ref[v, b]]
            blk_out[n >> 1] = b
            half_out[n] = 2 * place
            n = n + used
            blk_out[n >> 1] = b
            half_out[n] = 2 * place + 1
            n = n + jnp.where(count > 128, used, 0)
        half_out[n] = -1
        return n + (n & 1)

    end = lax.fori_loop(0, blocks, visits, I32(0)) >> 1

    def no_item(k, carry):
        blk_out[k] = blocks
        half_out[2 * k] = 0
        half_out[2 * k + 1] = -1
        return carry

    lax.fori_loop(end, end + PAD, no_item, 0)
    n_out[0] = end


def remote_kernel(n_ref, blk_ref, half_ref, nact_ref, fc_ref, tab_ref, acc_in_ref, key_ref, pos_ref, out_ref, acc_ref, sem, *flat):
    blocks = pos_ref.shape[1]
    copy = pltpu.make_async_copy(acc_in_ref, acc_ref, sem)
    copy.start()
    run_items(
        (n_ref[0] + KI - 1) // KI,
        blk_ref,
        half_ref,
        nact_ref,
        fc_ref,
        lambda one: tab_ref[one],
        acc_ref,
        take_buffers(flat),
        copy.wait,
    )

    def finish(bb, carry):
        for u in range(4):
            b = bb * 4 + u
            acc = acc_ref[b]
            top = acc[0:8]
            total = top + pltpu.roll(top, 4, 0) + acc[8:16]
            key = key_ref[pl.ds(b, 1), :]
            parts = []
            for h in range(2):
                at = jnp.broadcast_to(key[:, 128 * h : 128 * h + 128], (8, 128))
                lane = at & 127
                left = jnp.take_along_axis(total[:, :128], lane, axis=1, mode="promise_in_bounds")
                right = jnp.take_along_axis(total[:, 128:], lane, axis=1, mode="promise_in_bounds")
                parts.append(jnp.where(at < 128, left, right))
            back = jnp.concatenate(parts, axis=1)
            for c in range(3):
                pull = (back[c : c + 1] - pos_ref[c, pl.ds(b, 1), :] * back[3:4]) * LEAD
                out_ref[c, pl.ds(b, 1), :] = jnp.where(key >= 0, pull, 0.0)
        return carry

    lax.fori_loop(0, blocks // 4, finish, 0)


def forces_of(positions, time_bins, home_groups, targets, target_groups, node_pos, node_mass, node_lists, list_counts):
    domains = lax.axis_size("dom")
    sharers = lax.axis_size("sub")
    blocks, most = targets.shape
    pairs = blocks * most
    width = positions.shape[2]
    lists = node_lists.shape[0]
    rows = node_mass.shape[0] // 128

    asked = (targets.T, target_groups.T, list_counts.reshape(1, lists), node_pos, node_mass.reshape(1, -1), time_bins)
    req, slot, nact, nodes = pl.pallas_call(
        request_kernel,
        out_shape=(
            jax.ShapeDtypeStruct((domains, 128), I32),
            jax.ShapeDtypeStruct((1, pairs), I32),
            jax.ShapeDtypeStruct((1, blocks), I32),
            jax.ShapeDtypeStruct((4, rows, 128), F32),
        ),
        in_specs=[hspec()] * 6,
        out_specs=(vspec(),) * 4,
        scratch_shapes=[*[VMEM(a.shape, a.dtype) for a in asked], pltpu.SemaphoreType.DMA((6,))],
        compiler_params=pltpu.CompilerParams(vmem_limit_bytes=60 << 20),
        name="requests",
    )(*asked)
    held = [nodes]
    for j in range(1, sharers // 2):
        held.append(lax.ppermute(nodes, "sub", [(i, (i + 2 * j) % sharers) for i in range(sharers)]))
    req = lax.all_to_all(req.reshape(domains, 1, 128), "dom", 0, 0, tiled=True)
    req = req.reshape(domains, 128)
    nact = nact.reshape(blocks)

    mine = build_lists(held, node_lists, list_counts)
    theirs = lax.ppermute(mine, "sub", [(i, i ^ 1) for i in range(sharers)])
    reply = pl.pallas_call(
        pack_kernel,
        out_shape=jax.ShapeDtypeStruct((domains, SLOTS, 8, 128), F32),
        in_specs=[sspec(), vspec(), vspec()],
        out_specs=hspec(),
        scratch_shapes=[VMEM((domains, SLOTS, 8, 128), F32), pltpu.SemaphoreType.DMA((4,))],
        compiler_params=pltpu.CompilerParams(vmem_limit_bytes=60 << 20),
        name="pack",
    )(req, mine, theirs)
    reply = lax.all_to_all(reply.reshape(domains, SLOTS * 8, 128), "dom", 0, 0, tiled=True)

    positions = jnp.transpose(positions, (1, 0, 2))
    room = pairs + PAD
    fc, key, acc, blk, half, n = pl.pallas_call(
        home_kernel,
        out_shape=(
            jax.ShapeDtypeStruct((blocks, 32, width), BF16),
            jax.ShapeDtypeStruct((blocks, width), I32),
            jax.ShapeDtypeStruct((blocks + 1, 16, width), F32),
            jax.ShapeDtypeStruct((room,), I32),
            jax.ShapeDtypeStruct((2 * room,), I32),
            jax.ShapeDtypeStruct((8,), I32),
        ),
        in_specs=[sspec()] * 5 + [vspec()] * 4,
        out_specs=(vspec(),) * 3 + (sspec(),) * 3,
        scratch_shapes=[SMEM((blocks + PAD,), I32), SMEM((2 * (blocks + PAD),), I32), SMEM((blocks + 1,), I32), VMEM((4, width, width), BF16), *buffers()],
        compiler_params=pltpu.CompilerParams(vmem_limit_bytes=65136 << 10),
        cost_estimate=pl.CostEstimate(flops=40_000_000, bytes_accessed=4_000_000, transcendentals=12_000_000),
        name="home_pulls",
    )(home_groups, slot, target_groups.T, req, nact, positions, time_bins, mine, theirs)

    out = pl.pallas_call(
        remote_kernel,
        out_shape=jax.ShapeDtypeStruct((3, blocks, width), F32),
        in_specs=[sspec()] * 4 + [vspec(), vspec(), hspec(), vspec(), vspec()],
        out_specs=vspec(),
        scratch_shapes=[VMEM((blocks + 1, 16, width), F32), pltpu.SemaphoreType.DMA, *buffers()],
        compiler_params=pltpu.CompilerParams(vmem_limit_bytes=60 << 20),
        name="remote_pulls",
    )(n, blk, half, nact, fc, reply.reshape(domains * SLOTS, 8, 128), acc, key, positions)
    return jnp.transpose(out, (1, 0, 2))


def solution(mesh):
    return jax.shard_map(
        forces_of,
        mesh=mesh,
        in_specs=(
            P(("dom", "sub"), None, None),
            P(("dom", "sub"), None),
            P(("dom", "sub")),
            P(("dom", "sub"), None),
            P(("dom", "sub"), None),
            P(None, ("dom", "sub")),
            P(("dom", "sub")),
            P("dom", None),
            P("dom"),
        ),
        out_specs=P(("dom", "sub"), None, None),
        check_vma=False,
    )
```
